32 devices in a mesh: row: 4 (over y, x), col: 8 (over z, core).
Axes of the slice: x: 2, y: 2, z: 4, core: 2. Of those that a mesh axis runs over, the one named last changes fastest.
Arguments:
- pair_rep: bfloat16 [512, 512, 128], P('row', 'col'), may hold values from -6 to 6
- ln_gain: float32 [128], replicated, may hold values from 0.1 to 1.9
- ln_shift: float32 [128], replicated, may hold values from -3 to 3
- w_proj: bfloat16 [128, 512], replicated, may hold values from -0.5 to 0.5
- gate_bias: float32 [128], replicated, may hold values from -4 to 4
- w_bias: bfloat16 [128, 4], replicated, may hold values from -11 to 11
- w_out: bfloat16 [128, 128], replicated, may hold values from -0.5 to 0.5
- out_bias: float32 [128], replicated, may hold values from -3 to 3
- block_valid: int32 [4], replicated, may hold values from 0 to 1, as said below
Outputs:
- pair_out: bfloat16 [512, 512, 128], P('row', 'col')
The draws below stay inside these ranges and needn't reach their ends.
Inputs may be any that keep to these rules, and one draw needn't show every extreme that they name: block_valid[b] is 1 when residues b * 128 to (b + 1) * 128 - 1 are present and 0 when they are padding; blocks 0 and 2 are always present, and at least one other block is always padding.
All inputs are finite; a program needn't handle non-finite values.
Results may differ from the reference program's by a relative error of at most 0.0082.
Values may be sent and summed in bfloat16 or wider, within the bound.
No kernel may reach another device: no remote copies, remote signals or barrier semaphores. Data moves between devices by JAX's collectives and lax.ppermute only.
A program may use at most 192 MiB of HBM per device.

```python
import jax
import jax.numpy as jnp
from jax import lax

C = 128
H = 4
HD = 32
RES = 512
NBLK = 4


def draw_w_bias(key, part):
    base = jnp.clip(jax.random.normal(key, (C, H), jnp.float32), -4.0, 4.0) * 0.13
    return base.astype(jnp.bfloat16)


def draw_block_valid(key, part):
    places = jnp.arange(NBLK, dtype=jnp.int32)
    levels = jax.random.randint(key, (NBLK,), 0, 2, dtype=jnp.int32)
    bits = jnp.where(levels > 0, 1, 0).astype(jnp.int32)
    bits = jnp.where((places == 0) | (places == NBLK // 2), 1, bits)
    if NBLK >= 3:
        candidate = jax.random.randint(jax.random.fold_in(key, 7), (), 1, NBLK - 1, dtype=jnp.int32)
        padded = jnp.where(candidate == NBLK // 2, NBLK - 1, candidate).astype(jnp.int32)
        bits = jnp.where(places == padded, 0, bits)
    return bits.astype(jnp.int32)


def level_of(own_key, dims, pieces, low, high):
    level = 1.0
    for dim, blocks in pieces:
        steps = jax.random.uniform(jax.random.fold_in(jax.random.fold_in(own_key, 6), dim), (blocks,), jnp.float32, low / len(pieces), high / len(pieces))
        level = level * jnp.repeat(jnp.exp(steps), dims[dim] // blocks).reshape((-1,) + (1,) * (len(dims) - 1 - dim))
    return level


def noise(rng, dims, deviation, most, split=(), kind=jnp.bfloat16):
    gain = level_of(rng, dims, split, -0.22, 0.18) if split else 1.0
    values = jax.random.normal(rng, dims, jnp.float32) * deviation * gain
    return jnp.minimum(jnp.maximum(values, -most), most).astype(kind)


def setup_inputs(seed: int = 0) -> dict:
    arg_keys = jax.random.split(jax.random.key(seed), 10)
    return {
        "pair_rep": noise(arg_keys[0], (RES, RES, C), 1.0, 6.0, ((0, 4), (1, 8))),
        "ln_gain": jnp.clip(1.0 + 0.18 * jax.random.normal(arg_keys[1], (C,), jnp.float32), 0.1, 1.9),
        "ln_shift": noise(arg_keys[2], (C,), 0.5, 3.0, (), jnp.float32),
        "w_proj": noise(arg_keys[3], (C, 4 * H * HD), C ** -0.5, 0.5),
        "gate_bias": noise(arg_keys[4], (H * HD,), 1.0, 4.0, (), jnp.float32),
        "w_bias": draw_w_bias(jax.random.fold_in(arg_keys[9], 71), 0),
        "w_out": noise(arg_keys[6], (H * HD, C), (H * HD) ** -0.5, 0.5),
        "out_bias": noise(arg_keys[7], (C,), 0.5, 3.0, (), jnp.float32),
        "block_valid": draw_block_valid(jax.random.fold_in(arg_keys[9], 71), 0),
    }


def layer_norm(values, ln_gain, ln_shift):
    widened = values.astype(jnp.float32)
    average = lax.optimization_barrier(jnp.mean(widened, axis=-1, keepdims=True))
    spread = lax.optimization_barrier(jnp.mean((widened - average) ** 2, axis=-1, keepdims=True))
    return ((widened - average) * lax.rsqrt(spread + 1e-05) * ln_gain + ln_shift).astype(jnp.bfloat16)

def residue_valid(block_valid, residues):
    blocks = block_valid.shape[0]
    block_width = residues // blocks
    owner = jnp.arange(residues, dtype=jnp.int32) // block_width
    matches = (owner[:, None] == jnp.arange(blocks, dtype=jnp.int32)[None, :]).astype(jnp.float32)
    return lax.optimization_barrier(jnp.sum(matches * block_valid.astype(jnp.float32)[None, :], axis=1))

def reference(pair_rep, ln_gain, ln_shift, w_proj, gate_bias, w_bias, w_out, out_bias, block_valid):
    residues = pair_rep.shape[0]
    inner = H * HD
    validity = residue_valid(block_valid, residues)
    normed = lax.map(lambda row_in: layer_norm(row_in, ln_gain, ln_shift), pair_rep)
    bias_rows = lax.map(lambda row_in: jnp.dot(row_in, w_bias, preferred_element_type=jnp.float32), normed)
    bias_t = jnp.transpose(bias_rows, (2, 1, 0))

    def column(index):
        column_in = lax.dynamic_index_in_dim(normed, index, 1, keepdims=False)
        pair_col = lax.dynamic_index_in_dim(pair_rep, index, 1, keepdims=False)
        projected = jnp.dot(column_in, w_proj, preferred_element_type=jnp.float32)
        queries = (projected[:, :inner] * HD ** (-0.5)).astype(jnp.bfloat16)
        key_rows = projected[:, inner:2 * inner].astype(jnp.bfloat16)
        values = projected[:, 2 * inner:3 * inner].astype(jnp.bfloat16)
        gate_act = jax.nn.sigmoid(projected[:, 3 * inner:] + gate_bias)
        query_heads = queries.reshape(residues, H, HD).astype(jnp.float32)
        key_heads = key_rows.reshape(residues, H, HD).astype(jnp.float32)
        value_heads = values.reshape(residues, H, HD).astype(jnp.float32)
        scores = jnp.einsum('ihd,khd->hik', query_heads, key_heads) + bias_t
        scores = jnp.where(validity[None, None, :] > 0, scores, jnp.float32(-1e+30))
        row_max = lax.optimization_barrier(jnp.max(scores, axis=-1, keepdims=True))
        weights = jnp.exp(scores - row_max) * validity[None, None, :]
        denominator = lax.optimization_barrier(jnp.sum(weights, axis=-1))
        rounded = weights.astype(jnp.bfloat16).astype(jnp.float32)
        mixed = jnp.einsum('hik,khd->ihd', rounded, value_heads) / jnp.transpose(denominator)[:, :, None]
        attended = mixed.reshape(residues, inner).astype(jnp.bfloat16)
        gated_rows = (gate_act * attended.astype(jnp.float32)).astype(jnp.bfloat16)
        update = jnp.dot(gated_rows, w_out, preferred_element_type=jnp.float32) + out_bias
        col_valid = lax.dynamic_index_in_dim(validity, index, 0, keepdims=False)
        update = update * (validity * col_valid)[:, None]
        return (pair_col.astype(jnp.float32) + update).astype(jnp.bfloat16)
    results = lax.map(column, jnp.arange(residues, dtype=jnp.int32))
    return jnp.transpose(results, (1, 0, 2))
```

```python
import itertools
import math

import jax
import jax.numpy as jnp
from jax import lax
from jax.experimental import pallas as pl
from jax.experimental.pallas import tpu as pltpu
from jax.sharding import PartitionSpec as P

H = 4
HD = 32
BLK = 128


VMEM = pltpu.MemorySpace.VMEM
SMEM = pltpu.MemorySpace.SMEM
ANY = pl.ANY


def norm_kernel(x_ref, gain_ref, shift_ref, wb_ref, *rest):
    n_ref, bias_ref, scratch = rest[-3:]
    rows, cols, channels = x_ref.shape
    step = 16

    def norm_rows(index, carried):
        start = index * step
        widened = x_ref[pl.ds(start, step)].astype(jnp.float32)
        average = jnp.mean(widened, axis=-1, keepdims=True)
        centred = widened - average
        spread = jnp.mean(centred * centred, axis=-1, keepdims=True)
        out = centred * lax.rsqrt(spread + 1e-05) * gain_ref[...] + shift_ref[...]
        scratch[pl.ds(start * cols, step * cols), :] = out.reshape(step * cols, channels)
        return carried

    lax.fori_loop(0, rows // step, norm_rows, 0)
    for j in range(cols):
        column = scratch[pl.ds(j, rows, stride=cols), :].astype(jnp.bfloat16)
        n_ref[j] = column
        part = lax.dot_general(
            wb_ref[...], column, (((1,), (1,)), ((), ())), preferred_element_type=jnp.float32
        )
        for h in range(H):
            bias_ref[h, j : j + 1, :] = part[h : h + 1, :]


def norm_chunk(x, gain, shift, wb, bias_in, chunk, chunks):
    rows, cols_dev, channels = x.shape
    cols = cols_dev // chunks
    in_specs = [
        pl.BlockSpec((rows, cols, channels), lambda i: (0, chunk, 0)),
        pl.BlockSpec((1, channels), lambda i: (0, 0)),
        pl.BlockSpec((1, channels), lambda i: (0, 0)),
        pl.BlockSpec(wb.shape, lambda i: (0, 0)),
    ]
    operands = [x, gain, shift, wb]
    aliases = {}
    if bias_in is not None:
        in_specs.append(pl.BlockSpec(memory_space=ANY))
        operands.append(bias_in)
        aliases = {4: 1}
    return pl.pallas_call(
        norm_kernel,
        grid=(1,),
        in_specs=in_specs,
        out_specs=[
            pl.BlockSpec((cols, rows, channels), lambda i: (0, 0, 0)),
            pl.BlockSpec((H, cols, rows), lambda i: (0, chunk, 0)),
        ],
        out_shape=[
            jax.ShapeDtypeStruct((cols, rows, channels), jnp.bfloat16),
            jax.ShapeDtypeStruct((H, cols_dev, rows), jnp.float32),
        ],
        scratch_shapes=[pltpu.VMEM((rows * cols, channels), jnp.float32)],
        input_output_aliases=aliases,
        cost_estimate=pl.CostEstimate(flops=40 * rows * cols * channels, bytes_accessed=4 * rows * cols * channels, transcendentals=0),
        name="norm_%d" % chunk,
    )(*operands)


def attend_kernel(flags, x_ref, wqg_ref, wkv_ref, wout_ref, gb_ref, ob_ref, *rest, parts, inner_count):
    n_refs = rest[:parts]
    bias_refs = rest[parts : parts + inner_count]
    out_ref, scratch, bias_s, sem = rest[-4:]
    rows, cols, channels = x_ref.shape
    inner = H * HD
    keys = parts * rows
    active = flags[0] > 0

    @pl.when(active)
    def _():
        span = bias_refs[0].shape[1]
        copies = []
        for a in range(inner_count):
            offset = pl.multiple_of(flags[1 + a] * span, span)
            copy = pltpu.make_async_copy(bias_refs[a], bias_s.at[:, pl.ds(offset, span), :], sem.at[a])
            copy.start()
            copies.append(copy)
        for copy in copies:
            copy.wait()
        lane = lax.broadcasted_iota(jnp.int32, (1, inner), 1) // HD
        head_masks = [lane == h for h in range(H)]
        ones = [jnp.broadcast_to(jnp.where(m, 1.0, 0.0), (keys, inner)).astype(jnp.bfloat16) for m in head_masks]

        def column(j, carried):
            own = n_refs[0][j]
            qg = jnp.dot(own, wqg_ref[...], preferred_element_type=jnp.float32)
            q = (qg[:, :inner] * HD ** (-0.5)).astype(jnp.bfloat16)
            gate = jax.nn.sigmoid(qg[:, inner:] + gb_ref[...])
            stacked = jnp.concatenate([n_refs[u][j] for u in range(parts)], axis=0)
            kv = jnp.dot(stacked, wkv_ref[...], preferred_element_type=jnp.float32).astype(jnp.bfloat16)
            k = kv[:, :inner]
            v = kv[:, inner:]
            mixed = None
            zero = jnp.zeros((), jnp.bfloat16)
            for h in range(H):
                qh = jnp.where(head_masks[h], q, zero)
                s = lax.dot_general(qh, k, (((1,), (1,)), ((), ())), preferred_element_type=jnp.float32)
                s = s + bias_s[h]
                top = jnp.max(s, axis=-1, keepdims=True)
                w = jnp.exp(s - top).astype(jnp.bfloat16)
                vh = jnp.concatenate([jnp.where(head_masks[h], v, zero), ones[h]], axis=1)
                term = jnp.dot(w, vh, preferred_element_type=jnp.float32)
                mixed = term if mixed is None else mixed + term
            attended = (mixed[:, :inner] / mixed[:, inner:]).astype(jnp.bfloat16)
            gated = (gate * attended.astype(jnp.float32)).astype(jnp.bfloat16)
            update = jnp.dot(gated, wout_ref[...], preferred_element_type=jnp.float32) + ob_ref[...]
            scratch[pl.ds(j, rows, stride=cols), :] = update
            return carried

        lax.fori_loop(0, cols, column, 0)
        step = 16

        def finish(index, carried):
            start = index * step
            update = scratch[pl.ds(start * cols, step * cols), :].reshape(step, cols, channels)
            out_ref[pl.ds(start, step)] = (x_ref[pl.ds(start, step)].astype(jnp.float32) + update).astype(jnp.bfloat16)
            return carried

        lax.fori_loop(0, rows // step, finish, 0)

    @pl.when(jnp.logical_not(active))
    def _():
        out_ref[...] = x_ref[...]


def attend_chunk(flags, x, weights, norms, biases, out_in, chunk, chunks):
    rows, cols_dev, channels = x.shape
    cols = cols_dev // chunks
    parts = len(norms)
    keys = parts * rows
    inner_count = len(biases)
    span = biases[0].shape[1]
    whole = lambda a: pl.BlockSpec(a.shape, lambda i, f, nd=a.ndim: (0,) * nd)
    in_specs = [pl.BlockSpec((rows, cols, channels), lambda i, f: (0, chunk, 0))]
    in_specs += [whole(a) for a in weights] + [whole(a) for a in norms]
    in_specs += [pl.BlockSpec(memory_space=ANY) for _ in biases]
    operands = [flags, x, *weights, *norms, *biases]
    aliases = {}
    if out_in is not None:
        in_specs.append(pl.BlockSpec(memory_space=ANY))
        aliases = {len(operands): 0}
        operands.append(out_in)

    def body(flags_ref, *refs):
        attend_kernel(flags_ref, *refs, parts=parts, inner_count=inner_count)

    return pl.pallas_call(
        body,
        grid_spec=pltpu.PrefetchScalarGridSpec(
            num_scalar_prefetch=1,
            grid=(1,),
            in_specs=in_specs,
            out_specs=pl.BlockSpec((rows, cols, channels), lambda i, f: (0, chunk, 0)),
            scratch_shapes=[
                pltpu.VMEM((rows * cols, channels), jnp.float32),
                pltpu.VMEM((H, inner_count * span, keys), jnp.float32),
                pltpu.SemaphoreType.DMA((inner_count,)),
            ],
        ),
        out_shape=jax.ShapeDtypeStruct((rows, cols_dev, channels), jnp.bfloat16),
        input_output_aliases=aliases,
        cost_estimate=pl.CostEstimate(
            flops=4 * cols * H * rows * keys * 128, bytes_accessed=2 * cols * channels * (2 * rows + keys), transcendentals=cols * H * rows * keys
        ),
        name="attend_%d" % chunk,
    )(*operands)


def run_pattern(valid, row_count, col_count, args):
    pair_rep, ln_gain, ln_shift, w_proj, gate_bias, w_bias, w_out, out_bias = args
    rows_dev, cols_dev, channels = pair_rep.shape
    inner = H * HD
    group = rows_dev // cols_dev
    nv = len(valid)
    chunks = max(1, cols_dev // 16)
    row_id = lax.axis_index("row")
    col_id = lax.axis_index("col")
    block_id = col_id // group
    inner_id = col_id % group
    axes = ("row", "col")

    def at(row, block, a):
        return row * col_count + block * group + a

    gain = ln_gain.reshape(1, channels)
    shift = ln_shift.reshape(1, channels)
    wb = jnp.pad(w_bias.T, ((0, 8 - H), (0, 0)))
    wqg = jnp.concatenate([w_proj[:, :inner], w_proj[:, 3 * inner :]], axis=1)
    wkv = w_proj[:, inner : 3 * inner]
    weights = (wqg, wkv, w_out, gate_bias.reshape(1, inner), out_bias.reshape(1, channels))

    norms = []
    bias = None
    for c in range(chunks):
        n_c, bias = norm_chunk(pair_rep, gain, shift, wb, bias, c, chunks)
        norms.append(n_c)

    def send(x, moves):
        pairs = [(at(a, b, i), at(d, b, i)) for (a, d) in moves for b in valid for i in range(group)]
        return lax.ppermute(x, axes, pairs)

    pieces = [bias]
    for u in range(1, nv):
        pairs = []
        for p in range(nv):
            for i in range(group):
                pairs.append((at(valid[(p - u) % nv], valid[p], i), at(valid[p], valid[p], i)))
        pieces.append(lax.ppermute(bias, axes, pairs))
    stacked = jnp.concatenate(pieces, axis=2)
    chosen = stacked
    for t in range(1, nv):
        pairs = []
        mine = jnp.zeros((), jnp.bool_)
        for p in range(nv):
            target = valid[(p + t) % nv]
            mine = mine | ((row_id == valid[p]) & (block_id == target))
            for i in range(group):
                pairs.append((at(valid[p], valid[p], i), at(valid[p], target, i)))
        moved = lax.ppermute(stacked, axes, pairs)
        chosen = jnp.where(mine, moved, chosen)
    biases = [chosen]
    for a in range(1, group):
        pairs = [(at(r, b, i), at(r, b, (i + a) % group)) for r in valid for b in valid for i in range(group)]
        biases.append(lax.ppermute(chosen, axes, pairs))

    row_ok = jnp.zeros((), jnp.bool_)
    col_ok = jnp.zeros((), jnp.bool_)
    for b in valid:
        row_ok = row_ok | (row_id == b)
        col_ok = col_ok | (block_id == b)
    active = (row_ok & col_ok).astype(jnp.int32)
    flags = jnp.stack([active] + [((inner_id - a) % group).astype(jnp.int32) for a in range(group)])

    out = None
    for c in range(chunks):
        parts = [norms[c]]
        for u in range(1, nv):
            parts.append(send(norms[c], [(valid[(p - u) % nv], valid[p]) for p in range(nv)]))
        out = attend_chunk(flags, pair_rep, weights, parts, biases, out, c, chunks)
    return out


def patterns(blocks):
    fixed = {0, blocks // 2}
    free = [b for b in range(blocks) if b not in fixed]
    found = []
    for bits in itertools.product((0, 1), repeat=len(free)):
        if sum(bits) < len(free):
            found.append((bits, tuple(sorted(fixed | {b for b, on in zip(free, bits) if on}))))
    return free, found


def shards(pair_rep, ln_gain, ln_shift, w_proj, gate_bias, w_bias, w_out, out_bias, block_valid):
    row_count = lax.axis_size("row")
    col_count = lax.axis_size("col")
    args = (pair_rep, ln_gain, ln_shift, w_proj, gate_bias, w_bias, w_out, out_bias)
    free, found = patterns(block_valid.shape[0])
    index = jnp.zeros((), jnp.int32)
    for place, (bits, _) in enumerate(found):
        same = jnp.ones((), jnp.bool_)
        for b, on in zip(free, bits):
            same = same & ((block_valid[b] > 0) == bool(on))
        index = jnp.where(same, place, index)
    branches = [lambda ops, v=v: run_pattern(v, row_count, col_count, ops) for _, v in found]
    return lax.switch(index, branches, args)


def layer_norm(values, ln_gain, ln_shift):
    widened = values.astype(jnp.float32)
    average = jnp.mean(widened, axis=-1, keepdims=True)
    spread = jnp.mean((widened - average) ** 2, axis=-1, keepdims=True)
    return ((widened - average) * lax.rsqrt(spread + 1e-05) * ln_gain + ln_shift).astype(
        jnp.bfloat16
    )


def residue_valid(block_valid, residues):
    blocks = block_valid.shape[0]
    block_width = residues // blocks
    owner = jnp.arange(residues, dtype=jnp.int32) // block_width
    matches = (owner[:, None] == jnp.arange(blocks, dtype=jnp.int32)[None, :]).astype(jnp.float32)
    return jnp.sum(matches * block_valid.astype(jnp.float32)[None, :], axis=1)


def start_state(width_j, query_count):
    running_max = jnp.full((H, width_j, query_count), -1e30, jnp.float32)
    denominator = jnp.zeros((H, width_j, query_count), jnp.float32)
    weighted = jnp.zeros((query_count, width_j, H, HD), jnp.float32)
    return (running_max, denominator, weighted)


def finish(carried):
    running_max, denominator, weighted = carried
    mixed = weighted / jnp.transpose(denominator, (2, 1, 0))[..., None]
    return mixed.reshape(mixed.shape[0], mixed.shape[1], H * HD).astype(jnp.bfloat16)


def fold_keys(carried, queries, key_rows, values, bias_part, validity):
    query_count, width_j, inner = queries.shape
    key_count = key_rows.shape[0]
    key_step = math.gcd(key_count, BLK)
    steps = key_count // key_step
    query_heads = queries.reshape(query_count, width_j, H, HD)
    key_blocks = key_rows.reshape(steps, key_step, width_j, H, HD)
    value_blocks = values.reshape(steps, key_step, width_j, H, HD)
    bias_blocks = jnp.transpose(bias_part.reshape(H, query_count, steps, key_step), (2, 0, 1, 3))
    mask_blocks = validity.reshape(steps, key_step)

    def update(carried_in, operands):
        key_part, value_part, bias_block, mask_part = operands
        running_max, denominator, weighted = carried_in
        scores = jnp.einsum(
            "ijhd,kjhd->hjik", query_heads, key_part, preferred_element_type=jnp.float32
        )
        scores = scores + bias_block[:, None, :, :]
        scores = jnp.where(mask_part[None, None, None, :] > 0, scores, jnp.float32(-1e30))
        renewed = jnp.maximum(running_max, jnp.max(scores, axis=-1))
        weights = jnp.exp(scores - renewed[..., None]) * mask_part[None, None, None, :]
        shrink = jnp.exp(running_max - renewed)
        denominator = denominator * shrink + jnp.sum(weights, axis=-1)
        product = jnp.einsum(
            "hjik,kjhd->ijhd",
            weights.astype(jnp.bfloat16),
            value_part,
            preferred_element_type=jnp.float32,
        )
        weighted = weighted * jnp.transpose(shrink, (2, 1, 0))[..., None] + product
        return (renewed, denominator, weighted)

    def scan_step(carried_in, operands):
        renewed = lax.cond(
            jnp.max(operands[3]) > 0, update, lambda kept, ignored: kept, carried_in, operands
        )
        return (renewed, None)

    result, ignored = lax.scan(
        scan_step, carried, (key_blocks, value_blocks, bias_blocks, mask_blocks)
    )
    return result


def general_shards(pair_rep, ln_gain, ln_shift, w_proj, gate_bias, w_bias, w_out, out_bias, block_valid):
    rows_dev, cols_dev, channels = pair_rep.shape
    row_count = lax.axis_size("row")
    row_id = lax.axis_index("row")
    col_id = lax.axis_index("col")
    residues = rows_dev * row_count
    inner = H * HD
    query_scale = HD ** (-0.5)
    validity = residue_valid(block_valid, residues)
    normed = layer_norm(pair_rep, ln_gain, ln_shift)
    flat_rows = normed.reshape(rows_dev * cols_dev, channels)
    bias_local = jnp.dot(flat_rows, w_bias, preferred_element_type=jnp.float32)
    bias_local = jnp.transpose(bias_local.reshape(rows_dev, cols_dev, H), (2, 1, 0))
    bias_cols = lax.all_gather(bias_local, "row", axis=2, tiled=True)
    regrouped = lax.all_to_all(normed, "row", split_axis=1, concat_axis=0, tiled=True)
    width_j = regrouped.shape[1]
    projected = jnp.dot(
        regrouped.reshape(residues * width_j, channels),
        w_proj[:, : 3 * inner],
        preferred_element_type=jnp.float32,
    )
    projected = projected.reshape(residues, width_j, 3 * inner)
    queries = (projected[..., :inner] * query_scale).astype(jnp.bfloat16)
    key_rows = projected[..., inner : 2 * inner].astype(jnp.bfloat16)
    values = projected[..., 2 * inner :].astype(jnp.bfloat16)
    bias_piece = lax.all_gather(bias_cols, "col", axis=1, tiled=True)
    span_rows = bias_piece.shape[1]
    query_block = math.gcd(span_rows, cols_dev)
    block_count = span_rows // query_block
    query_rows = queries
    query_rows = query_rows.reshape(block_count, query_block, width_j, inner)
    bias_blocks = jnp.transpose(
        bias_piece.reshape(H, block_count, query_block, residues), (1, 0, 2, 3)
    )

    def one_block(operands):
        query_part, bias_part = operands
        carried = fold_keys(
            start_state(width_j, query_block), query_part, key_rows, values, bias_part, validity
        )
        return finish(carried)

    results = lax.map(one_block, (query_rows, bias_blocks))
    gathered = results.reshape(span_rows, width_j, inner)
    attended = lax.all_to_all(gathered, "row", split_axis=0, concat_axis=1, tiled=True)
    gate_pre = jnp.dot(flat_rows, w_proj[:, 3 * inner :], preferred_element_type=jnp.float32)
    gate_pre = gate_pre.reshape(rows_dev, cols_dev, inner)
    gate_act = jax.nn.sigmoid(gate_pre + gate_bias)
    gated_rows = (gate_act * attended.astype(jnp.float32)).astype(jnp.bfloat16)
    update = jnp.dot(
        gated_rows.reshape(rows_dev * cols_dev, inner), w_out, preferred_element_type=jnp.float32
    )
    update = update.reshape(rows_dev, cols_dev, channels) + out_bias
    row_valid = lax.dynamic_slice_in_dim(validity, row_id * rows_dev, rows_dev, 0)
    col_valid = lax.dynamic_slice_in_dim(validity, col_id * cols_dev, cols_dev, 0)
    pair_mask = row_valid[:, None] * col_valid[None, :]
    return (pair_rep.astype(jnp.float32) + update * pair_mask[..., None]).astype(jnp.bfloat16)


def solution(mesh):
    def body(*args):
        pair_rep, block_valid = args[0], args[-1]
        blocks = block_valid.shape[0]
        rows_dev, cols_dev, _ = pair_rep.shape
        aligned = blocks == lax.axis_size("row") and rows_dev % cols_dev == 0 and cols_dev % 16 == 0
        if aligned and len(patterns(blocks)[1]) <= 4:
            return shards(*args)
        return general_shards(*args)

    return jax.shard_map(
        body,
        mesh=mesh,
        in_specs=(P("row", "col", None), P(), P(), P(), P(), P(), P(), P(), P()),
        out_specs=P("row", "col", None),
        check_vma=False,
    )
```

```python
import itertools
import math

import jax
import jax.numpy as jnp
from jax import lax
from jax.experimental import pallas as pl
from jax.experimental.pallas import tpu as pltpu
from jax.sharding import PartitionSpec as P

H = 4
HD = 32
BLK = 128


ANY = pl.ANY
NT = (((1,), (1,)), ((), ()))
TN = (((0,), (0,)), ((), ()))
F32 = jnp.float32
BF16 = jnp.bfloat16
SUB = 8


def norm_kernel(x_ref, gain_ref, shift_ref, wb_ref, *rest):
    n_ref, bias_ref, scratch = rest[-3:]
    rows, cols, channels = x_ref.shape
    step = 8
    count = rows // step
    centred = {}
    spread = {}
    for t in range(count + 2):
        if t < count:
            widened = x_ref[t * step : (t + 1) * step].reshape(step * cols, channels).astype(F32)
            centred[t] = widened - jnp.mean(widened, axis=-1, keepdims=True)
        if 0 <= t - 1 < count:
            spread[t - 1] = jnp.mean(centred[t - 1] * centred[t - 1], axis=-1, keepdims=True)
        if 0 <= t - 2 < count:
            scaled = centred.pop(t - 2) * lax.rsqrt(spread.pop(t - 2) + 1e-05)
            scratch[(t - 2) * step * cols : (t - 1) * step * cols, :] = scaled * gain_ref[...] + shift_ref[...]
    for j in range(cols):
        column = scratch[pl.ds(j, rows, stride=cols), :].astype(BF16)
        n_ref[j] = column
        part = lax.dot_general(wb_ref[...], column, NT, preferred_element_type=F32)
        for h in range(H):
            bias_ref[h, j : j + 1, :] = part[h : h + 1, :]


def norm_chunk(x, gain, shift, wb, bias_in, first, cols):
    rows, cols_dev, channels = x.shape
    sub = 16 if cols % 16 == 0 and first % 16 == 0 else SUB
    steps = cols // sub
    base = first // sub
    in_specs = [
        pl.BlockSpec((rows, sub, channels), lambda i: (0, base + i, 0)),
        pl.BlockSpec((1, channels), lambda i: (0, 0)),
        pl.BlockSpec((1, channels), lambda i: (0, 0)),
        pl.BlockSpec(wb.shape, lambda i: (0, 0)),
    ]
    operands = [x, gain, shift, wb]
    aliases = {}
    if bias_in is not None:
        in_specs.append(pl.BlockSpec(memory_space=ANY))
        operands.append(bias_in)
        aliases = {4: 1}
    return pl.pallas_call(
        norm_kernel,
        grid=(steps,),
        in_specs=in_specs,
        out_specs=[
            pl.BlockSpec((sub, rows, channels), lambda i: (i, 0, 0)),
            pl.BlockSpec((H, sub, rows), lambda i: (0, base + i, 0)),
        ],
        out_shape=[
            jax.ShapeDtypeStruct((cols, rows, channels), BF16),
            jax.ShapeDtypeStruct((H, cols_dev, rows), F32),
        ],
        scratch_shapes=[pltpu.VMEM((rows * sub, channels), F32)],
        input_output_aliases=aliases,
        cost_estimate=pl.CostEstimate(
            flops=200 * rows * cols * channels, bytes_accessed=4 * rows * cols * channels, transcendentals=0
        ),
        name="norm_%d" % first,
    )(*operands)


def turn_kernel(flags, *refs, parts, group):
    out_ref, scratch = refs[-2:]
    span = refs[0].shape[1]
    rows = refs[0].shape[2]
    for u in range(parts):
        for h in range(H):
            for a in range(group):
                offset = pl.multiple_of(flags[1 + a] * span, span)
                scratch[pl.ds(offset, span), :] = refs[a * parts + u][h]
            out_ref[h, u * rows : (u + 1) * rows, :] = scratch[...].T


def turn(flags, pieces, parts, group):
    span, rows = pieces[0].shape[1:]

    def body(flags_ref, *refs):
        turn_kernel(flags_ref, *refs, parts=parts, group=group)

    return pl.pallas_call(
        body,
        grid_spec=pltpu.PrefetchScalarGridSpec(
            num_scalar_prefetch=1,
            grid=(1,),
            in_specs=[pl.BlockSpec(p.shape, lambda i, f: (0, 0, 0)) for p in pieces],
            out_specs=pl.BlockSpec((H, parts * rows, group * span), lambda i, f: (0, 0, 0)),
            scratch_shapes=[pltpu.VMEM((group * span, rows), F32)],
        ),
        out_shape=jax.ShapeDtypeStruct((H, parts * rows, group * span), F32),
        name="turn",
    )(flags, *pieces)


def attend_kernel(flags, x_ref, wqgv_ref, wk_ref, wout_ref, gb_ref, ob_ref, *rest, parts, aliased):
    n_refs = rest[:parts]
    bias_ref = rest[parts]
    rest = rest[parts + 1 + aliased :]
    out_ref, update_s, q_s, g_s, k_s, v_s, a_s, s_even, s_odd, p_even, p_odd = rest
    s_s = (s_even, s_odd)
    p_s = (p_even, p_odd)
    rows, cols, channels = x_ref.shape
    inner = H * HD
    keys = parts * rows
    wide = 2 * rows
    active = flags[0] > 0

    def project(t):
        own = n_refs[0][2 * t : 2 * t + 2].reshape(wide, channels)
        made = lax.dot_general(wqgv_ref[...], own, NT, preferred_element_type=F32)
        for e in range(2):
            lanes = slice(e * rows, (e + 1) * rows)
            q_s[2 * t + e] = (made[:inner, lanes] * HD ** (-0.5)).astype(BF16)
            g_s[2 * t + e] = jax.nn.sigmoid(made[inner : 2 * inner, lanes] + gb_ref[...])
            v_s[2 * t + e, :, 0:rows] = made[2 * inner :, lanes].astype(BF16)
        for u in range(1, parts):
            other = n_refs[u][2 * t : 2 * t + 2].reshape(wide, channels)
            made = lax.dot_general(wqgv_ref[2 * inner :], other, NT, preferred_element_type=F32)
            for e in range(2):
                v_s[2 * t + e, :, u * rows : (u + 1) * rows] = made[:, e * rows : (e + 1) * rows].astype(BF16)
        for u in range(parts):
            block = n_refs[u][2 * t : 2 * t + 2].reshape(wide, channels)
            made = jnp.dot(block, wk_ref[...], preferred_element_type=F32).astype(BF16)
            for e in range(2):
                k_s[2 * t + e, u * rows : (u + 1) * rows, :] = made[e * rows : (e + 1) * rows]

    def score(j, pair):
        q = q_s[j]
        columns = []
        for h in (2 * pair, 2 * pair + 1):
            blocks = [q[h * HD : (h + 1) * HD]]
            if h:
                blocks.insert(0, jnp.zeros((h * HD, rows), BF16))
            if h < H - 1:
                blocks.append(jnp.zeros(((H - 1 - h) * HD, rows), BF16))
            columns.append(jnp.concatenate(blocks, axis=0))
        both = jnp.concatenate(columns, axis=1)
        s_s[j % 2][:, pair * wide : (pair + 1) * wide] = jnp.dot(k_s[j], both, preferred_element_type=F32)

    def soften(j, h):
        scores = s_s[j % 2][:, h * rows : (h + 1) * rows] + bias_ref[h]
        top = jnp.max(scores, axis=0, keepdims=True)
        p_s[j % 2][:, h * rows : (h + 1) * rows] = jnp.exp(scores - top).astype(BF16)

    def mix(j, pair):
        lifted = jnp.concatenate([v_s[j, wide_head(pair)], jnp.ones((16, keys), BF16)], axis=0)
        mixed = jnp.dot(lifted, p_s[j % 2][:, pair * wide : (pair + 1) * wide], preferred_element_type=F32)
        for e in range(2):
            h = 2 * pair + e
            lanes = slice(e * rows, (e + 1) * rows)
            part = mixed[e * HD : (e + 1) * HD, lanes] / mixed[2 * HD : 2 * HD + 1, lanes]
            a_s[j, h * HD : (h + 1) * HD] = part.astype(BF16)

    def wide_head(pair):
        return slice(2 * pair * HD, (2 * pair + 2) * HD)

    def close(j):
        gated = (g_s[j] * a_s[j].astype(F32)).astype(BF16)
        update = lax.dot_general(gated, wout_ref[...], TN, preferred_element_type=F32) + ob_ref[...]
        update_s[pl.ds(j, rows, stride=cols), :] = update

    @pl.when(active)
    def _():
        for t in range(cols // 2):
            project(t)
        for t in range(-1, cols + 2):
            for pair in range(H // 2):
                if 0 <= t + 1 < cols:
                    score(t + 1, pair)
                if 0 <= t < cols:
                    soften(t, 2 * pair)
                    soften(t, 2 * pair + 1)
                if 0 <= t - 1 < cols:
                    mix(t - 1, pair)
            if 0 <= t - 2 < cols:
                close(t - 2)
        step = 16

        def finish(index, carried):
            start = index * step
            update = update_s[pl.ds(start * cols, step * cols), :].reshape(step, cols, channels)
            out_ref[pl.ds(start, step)] = (x_ref[pl.ds(start, step)].astype(F32) + update).astype(BF16)
            return carried

        lax.fori_loop(0, rows // step, finish, 0, unroll=2)

    @pl.when(jnp.logical_not(active))
    def _():
        out_ref[...] = x_ref[...]


def attend_chunk(flags, x, weights, norms, bias, out_in, first, cols):
    rows, cols_dev, channels = x.shape
    inner = H * HD
    parts = len(norms)
    keys = parts * rows
    steps = cols // SUB
    base = first // SUB
    whole = lambda a: pl.BlockSpec(a.shape, lambda i, f, nd=a.ndim: (0,) * nd)
    in_specs = [pl.BlockSpec((rows, SUB, channels), lambda i, f: (0, base + i, 0))]
    in_specs += [whole(a) for a in weights]
    in_specs += [pl.BlockSpec((SUB, rows, channels), lambda i, f: (i, 0, 0)) for _ in norms]
    in_specs.append(whole(bias))
    operands = [flags, x, *weights, *norms, bias]
    aliases = {}
    if out_in is not None:
        in_specs.append(pl.BlockSpec(memory_space=ANY))
        aliases = {len(operands): 0}
        operands.append(out_in)
    aliased = len(aliases)

    def body(flags_ref, *refs):
        attend_kernel(flags_ref, *refs, parts=parts, aliased=aliased)

    return pl.pallas_call(
        body,
        grid_spec=pltpu.PrefetchScalarGridSpec(
            num_scalar_prefetch=1,
            grid=(steps,),
            in_specs=in_specs,
            out_specs=pl.BlockSpec((rows, SUB, channels), lambda i, f: (0, base + i, 0)),
            scratch_shapes=[
                pltpu.VMEM((rows * SUB, channels), F32),
                pltpu.VMEM((SUB, inner, rows), BF16),
                pltpu.VMEM((SUB, inner, rows), F32),
                pltpu.VMEM((SUB, keys, inner), BF16),
                pltpu.VMEM((SUB, inner, keys), BF16),
                pltpu.VMEM((SUB, inner, rows), BF16),
                pltpu.VMEM((keys, H * rows), F32),
                pltpu.VMEM((keys, H * rows), F32),
                pltpu.VMEM((keys, H * rows), BF16),
                pltpu.VMEM((keys, H * rows), BF16),
            ],
        ),
        out_shape=jax.ShapeDtypeStruct((rows, cols_dev, channels), BF16),
        input_output_aliases=aliases,
        cost_estimate=pl.CostEstimate(
            flops=16 * cols * H * rows * keys * 128,
            bytes_accessed=2 * cols * channels * (2 * rows + keys),
            transcendentals=cols * H * rows * keys,
        ),
        name="attend_%d" % first,
    )(*operands)


def run_pattern(valid, row_count, col_count, args):
    pair_rep, ln_gain, ln_shift, w_proj, gate_bias, w_bias, w_out, out_bias = args
    rows_dev, cols_dev, channels = pair_rep.shape
    inner = H * HD
    group = rows_dev // cols_dev
    nv = len(valid)
    row_id = lax.axis_index("row")
    col_id = lax.axis_index("col")
    block_id = col_id // group
    inner_id = col_id % group
    axes = ("row", "col")

    def at(row, block, a):
        return row * col_count + block * group + a

    def move(x, pairs, blocks=valid):
        full = [(at(s, b, i), at(d, b, i)) for (s, d) in pairs for b in blocks for i in range(group)]
        return lax.ppermute(x, axes, full)

    row_ok = jnp.zeros((), jnp.bool_)
    col_ok = jnp.zeros((), jnp.bool_)
    row_place = jnp.zeros((), jnp.int32)
    block_place = jnp.zeros((), jnp.int32)
    for p, b in enumerate(valid):
        row_ok = row_ok | (row_id == b)
        col_ok = col_ok | (block_id == b)
        row_place = jnp.where(row_id == b, p, row_place)
        block_place = jnp.where(block_id == b, p, block_place)
    active = (row_ok & col_ok).astype(jnp.int32)
    flags = jnp.stack([active] + [((inner_id - a) % group).astype(jnp.int32) for a in range(group)])

    gain = ln_gain.reshape(1, channels)
    shift = ln_shift.reshape(1, channels)
    wb = jnp.pad(w_bias.T, ((0, 8 - H), (0, 0)))
    wqgv = jnp.concatenate([w_proj[:, :inner], w_proj[:, 3 * inner :], w_proj[:, 2 * inner : 3 * inner]], axis=1).T
    wk = w_proj[:, inner : 2 * inner]
    weights = (wqgv, wk, w_out, gate_bias.reshape(inner, 1), out_bias.reshape(1, channels))

    chunks = chunk_list(cols_dev)
    norms = []
    bias = None
    for first, cols in chunks:
        n_c, bias = norm_chunk(pair_rep, gain, shift, wb, bias, first, cols)
        norms.append(n_c)

    held = [bias]
    for t in range(1, nv):
        pairs = []
        for p in range(nv):
            for r in valid:
                for i in range(group):
                    pairs.append((at(r, valid[p], i), at(r, valid[(p + t) % nv], i)))
        held.append(lax.ppermute(bias, axes, pairs))

    def pick(place):
        back = (block_place - place) % nv
        chosen = held[0]
        for t in range(1, nv):
            chosen = jnp.where(back == t, held[t], chosen)
        return chosen

    picked = [pick((row_place + u) % nv) for u in range(nv)]
    pieces = [picked[0]]
    for u in range(1, nv):
        pairs = [(valid[p], valid[(p + u) % nv]) for p in range(nv)]
        pieces.append(move(picked[u], pairs))
    gathered = list(pieces)
    for a in range(1, group):
        pairs = [(at(r, b, i), at(r, b, (i + a) % group)) for r in valid for b in valid for i in range(group)]
        gathered += [lax.ppermute(piece, axes, pairs) for piece in pieces]
    bias_t = turn(flags, gathered, nv, group)

    square = row_count == 4
    ring = [[(valid[p], valid[(p + u) % nv]) for p in range(nv)] for u in range(nv)]
    parts = [[n_c] for n_c in norms]
    for index in range(len(chunks)):
        source = after(norms[index], picked[-1]) if index else norms[index]
        for u in range(1, nv):
            late = [(s, d) for s, d in ring[u] if square and (s ^ d) == 3 and (s ^ 1) in valid]
            if late:
                there = [(s, s ^ 2) if (s, d) in late else (s, d) for s, d in ring[u]]
                back = [(s ^ 2, d) if (s, d) in late else (d, d) for s, d in ring[u]]
                got = move(source, there)
                parts[index].append(move(after(got, bias_t if index else picked[-1]), back))
            else:
                parts[index].append(move(source, ring[u]))

    out = None
    for index, (first, cols) in enumerate(chunks):
        out = attend_chunk(flags, pair_rep, weights, parts[index], bias_t, out, first, cols)
    return out


def chunk_list(cols_dev):
    lengths = [cols_dev // 2, cols_dev // 2]
    if any(length % SUB for length in lengths):
        lengths = [16] * (cols_dev // 16)
    return [(sum(lengths[:i]), length) for i, length in enumerate(lengths)]


def after(value, *others):
    return lax.optimization_barrier((value, *others))[0] if others else value


def patterns(blocks):
    fixed = {0, blocks // 2}
    free = [b for b in range(blocks) if b not in fixed]
    found = []
    for bits in itertools.product((0, 1), repeat=len(free)):
        if sum(bits) < len(free):
            found.append((bits, tuple(sorted(fixed | {b for b, on in zip(free, bits) if on}))))
    return free, found


def shards(pair_rep, ln_gain, ln_shift, w_proj, gate_bias, w_bias, w_out, out_bias, block_valid):
    row_count = lax.axis_size("row")
    col_count = lax.axis_size("col")
    args = (pair_rep, ln_gain, ln_shift, w_proj, gate_bias, w_bias, w_out, out_bias)
    free, found = patterns(block_valid.shape[0])
    index = jnp.zeros((), jnp.int32)
    for place, (bits, _) in enumerate(found):
        same = jnp.ones((), jnp.bool_)
        for b, on in zip(free, bits):
            same = same & ((block_valid[b] > 0) == bool(on))
        index = jnp.where(same, place, index)
    branches = [lambda ops, v=v: run_pattern(v, row_count, col_count, ops) for _, v in found]
    return lax.switch(index, branches, args)


def layer_norm(values, ln_gain, ln_shift):
    widened = values.astype(jnp.float32)
    average = jnp.mean(widened, axis=-1, keepdims=True)
    spread = jnp.mean((widened - average) ** 2, axis=-1, keepdims=True)
    return ((widened - average) * lax.rsqrt(spread + 1e-05) * ln_gain + ln_shift).astype(
        jnp.bfloat16
    )


def residue_valid(block_valid, residues):
    blocks = block_valid.shape[0]
    block_width = residues // blocks
    owner = jnp.arange(residues, dtype=jnp.int32) // block_width
    matches = (owner[:, None] == jnp.arange(blocks, dtype=jnp.int32)[None, :]).astype(jnp.float32)
    return jnp.sum(matches * block_valid.astype(jnp.float32)[None, :], axis=1)


def start_state(width_j, query_count):
    running_max = jnp.full((H, width_j, query_count), -1e30, jnp.float32)
    denominator = jnp.zeros((H, width_j, query_count), jnp.float32)
    weighted = jnp.zeros((query_count, width_j, H, HD), jnp.float32)
    return (running_max, denominator, weighted)


def finish(carried):
    running_max, denominator, weighted = carried
    mixed = weighted / jnp.transpose(denominator, (2, 1, 0))[..., None]
    return mixed.reshape(mixed.shape[0], mixed.shape[1], H * HD).astype(jnp.bfloat16)


def fold_keys(carried, queries, key_rows, values, bias_part, validity):
    query_count, width_j, inner = queries.shape
    key_count = key_rows.shape[0]
    key_step = math.gcd(key_count, BLK)
    steps = key_count // key_step
    query_heads = queries.reshape(query_count, width_j, H, HD)
    key_blocks = key_rows.reshape(steps, key_step, width_j, H, HD)
    value_blocks = values.reshape(steps, key_step, width_j, H, HD)
    bias_blocks = jnp.transpose(bias_part.reshape(H, query_count, steps, key_step), (2, 0, 1, 3))
    mask_blocks = validity.reshape(steps, key_step)

    def update(carried_in, operands):
        key_part, value_part, bias_block, mask_part = operands
        running_max, denominator, weighted = carried_in
        scores = jnp.einsum(
            "ijhd,kjhd->hjik", query_heads, key_part, preferred_element_type=jnp.float32
        )
        scores = scores + bias_block[:, None, :, :]
        scores = jnp.where(mask_part[None, None, None, :] > 0, scores, jnp.float32(-1e30))
        renewed = jnp.maximum(running_max, jnp.max(scores, axis=-1))
        weights = jnp.exp(scores - renewed[..., None]) * mask_part[None, None, None, :]
        shrink = jnp.exp(running_max - renewed)
        denominator = denominator * shrink + jnp.sum(weights, axis=-1)
        product = jnp.einsum(
            "hjik,kjhd->ijhd",
            weights.astype(jnp.bfloat16),
            value_part,
            preferred_element_type=jnp.float32,
        )
        weighted = weighted * jnp.transpose(shrink, (2, 1, 0))[..., None] + product
        return (renewed, denominator, weighted)

    def scan_step(carried_in, operands):
        renewed = lax.cond(
            jnp.max(operands[3]) > 0, update, lambda kept, ignored: kept, carried_in, operands
        )
        return (renewed, None)

    result, ignored = lax.scan(
        scan_step, carried, (key_blocks, value_blocks, bias_blocks, mask_blocks)
    )
    return result


def general_shards(pair_rep, ln_gain, ln_shift, w_proj, gate_bias, w_bias, w_out, out_bias, block_valid):
    rows_dev, cols_dev, channels = pair_rep.shape
    row_count = lax.axis_size("row")
    row_id = lax.axis_index("row")
    col_id = lax.axis_index("col")
    residues = rows_dev * row_count
    inner = H * HD
    query_scale = HD ** (-0.5)
    validity = residue_valid(block_valid, residues)
    normed = layer_norm(pair_rep, ln_gain, ln_shift)
    flat_rows = normed.reshape(rows_dev * cols_dev, channels)
    bias_local = jnp.dot(flat_rows, w_bias, preferred_element_type=jnp.float32)
    bias_local = jnp.transpose(bias_local.reshape(rows_dev, cols_dev, H), (2, 1, 0))
    bias_cols = lax.all_gather(bias_local, "row", axis=2, tiled=True)
    regrouped = lax.all_to_all(normed, "row", split_axis=1, concat_axis=0, tiled=True)
    width_j = regrouped.shape[1]
    projected = jnp.dot(
        regrouped.reshape(residues * width_j, channels),
        w_proj[:, : 3 * inner],
        preferred_element_type=jnp.float32,
    )
    projected = projected.reshape(residues, width_j, 3 * inner)
    queries = (projected[..., :inner] * query_scale).astype(jnp.bfloat16)
    key_rows = projected[..., inner : 2 * inner].astype(jnp.bfloat16)
    values = projected[..., 2 * inner :].astype(jnp.bfloat16)
    bias_piece = lax.all_gather(bias_cols, "col", axis=1, tiled=True)
    span_rows = bias_piece.shape[1]
    query_block = math.gcd(span_rows, cols_dev)
    block_count = span_rows // query_block
    query_rows = queries
    query_rows = query_rows.reshape(block_count, query_block, width_j, inner)
    bias_blocks = jnp.transpose(
        bias_piece.reshape(H, block_count, query_block, residues), (1, 0, 2, 3)
    )

    def one_block(operands):
        query_part, bias_part = operands
        carried = fold_keys(
            start_state(width_j, query_block), query_part, key_rows, values, bias_part, validity
        )
        return finish(carried)

    results = lax.map(one_block, (query_rows, bias_blocks))
    gathered = results.reshape(span_rows, width_j, inner)
    attended = lax.all_to_all(gathered, "row", split_axis=0, concat_axis=1, tiled=True)
    gate_pre = jnp.dot(flat_rows, w_proj[:, 3 * inner :], preferred_element_type=jnp.float32)
    gate_pre = gate_pre.reshape(rows_dev, cols_dev, inner)
    gate_act = jax.nn.sigmoid(gate_pre + gate_bias)
    gated_rows = (gate_act * attended.astype(jnp.float32)).astype(jnp.bfloat16)
    update = jnp.dot(
        gated_rows.reshape(rows_dev * cols_dev, inner), w_out, preferred_element_type=jnp.float32
    )
    update = update.reshape(rows_dev, cols_dev, channels) + out_bias
    row_valid = lax.dynamic_slice_in_dim(validity, row_id * rows_dev, rows_dev, 0)
    col_valid = lax.dynamic_slice_in_dim(validity, col_id * cols_dev, cols_dev, 0)
    pair_mask = row_valid[:, None] * col_valid[None, :]
    return (pair_rep.astype(jnp.float32) + update * pair_mask[..., None]).astype(jnp.bfloat16)


def solution(mesh):
    def body(*args):
        pair_rep, block_valid = args[0], args[-1]
        blocks = block_valid.shape[0]
        rows_dev, cols_dev, _ = pair_rep.shape
        aligned = blocks == lax.axis_size("row") and rows_dev % cols_dev == 0 and cols_dev % 16 == 0
        if aligned and len(patterns(blocks)[1]) <= 4:
            return shards(*args)
        return general_shards(*args)

    return jax.shard_map(
        body,
        mesh=mesh,
        in_specs=(P("row", "col", None), P(), P(), P(), P(), P(), P(), P(), P()),
        out_specs=P("row", "col", None),
        check_vma=False,
    )
```

```python
import itertools
import math

import jax
import jax.numpy as jnp
from jax import lax
from jax.experimental import pallas as pl
from jax.experimental.pallas import tpu as pltpu
from jax.sharding import PartitionSpec as P


H = 4
HD = 32
BLK = 128


ANY = pl.ANY
NT = (((1,), (1,)), ((), ()))
TN = (((0,), (0,)), ((), ()))
F32 = jnp.float32
BF16 = jnp.bfloat16
SUB = 8
EIGHTHS = {2: (3, 3, 2), 3: (4, 4)}


def norm_kernel(x_ref, gain_ref, shift_ref, wb_ref, *rest):
    n_ref, bias_ref, scratch = rest[-3:]
    rows, cols, channels = x_ref.shape
    step = 8
    count = rows // step
    centred = {}
    spread = {}
    for t in range(count + 2):
        if t < count:
            widened = x_ref[t * step : (t + 1) * step].reshape(step * cols, channels).astype(F32)
            centred[t] = widened - jnp.mean(widened, axis=-1, keepdims=True)
        if 0 <= t - 1 < count:
            spread[t - 1] = jnp.mean(centred[t - 1] * centred[t - 1], axis=-1, keepdims=True)
        if 0 <= t - 2 < count:
            scaled = centred.pop(t - 2) * lax.rsqrt(spread.pop(t - 2) + 1e-05)
            scratch[(t - 2) * step * cols : (t - 1) * step * cols, :] = scaled * gain_ref[...] + shift_ref[...]
    for j in range(cols):
        column = scratch[pl.ds(j, rows, stride=cols), :].astype(BF16)
        n_ref[j] = column
        part = lax.dot_general(wb_ref[...], column, NT, preferred_element_type=F32)
        for h in range(H):
            bias_ref[h, j : j + 1, :] = part[h : h + 1, :]


def norm_chunk(x, gain, shift, wb, bias_in, first, cols):
    rows, cols_dev, channels = x.shape
    sub = 16 if cols % 16 == 0 and first % 16 == 0 else SUB
    steps = cols // sub
    base = first // sub
    in_specs = [
        pl.BlockSpec((rows, sub, channels), lambda i: (0, base + i, 0)),
        pl.BlockSpec((1, channels), lambda i: (0, 0)),
        pl.BlockSpec((1, channels), lambda i: (0, 0)),
        pl.BlockSpec(wb.shape, lambda i: (0, 0)),
    ]
    operands = [x, gain, shift, wb]
    aliases = {}
    if bias_in is not None:
        in_specs.append(pl.BlockSpec(memory_space=ANY))
        operands.append(bias_in)
        aliases = {4: 1}
    return pl.pallas_call(
        norm_kernel,
        grid=(steps,),
        in_specs=in_specs,
        out_specs=[
            pl.BlockSpec((sub, rows, channels), lambda i: (i, 0, 0)),
            pl.BlockSpec((H, sub, rows), lambda i: (0, base + i, 0)),
        ],
        out_shape=[
            jax.ShapeDtypeStruct((cols, rows, channels), BF16),
            jax.ShapeDtypeStruct((H, cols_dev, rows), F32),
        ],
        scratch_shapes=[pltpu.VMEM((rows * sub, channels), F32)],
        input_output_aliases=aliases,
        cost_estimate=pl.CostEstimate(
            flops=200 * rows * cols * channels, bytes_accessed=4 * rows * cols * channels, transcendentals=0
        ),
    )(*operands)


def turn_kernel(flags, *refs, parts, group):
    out_ref, scratch = refs[-2:]
    span, rows = refs[0].shape[1:]
    for u in range(parts):
        for h in range(H):
            for a in range(group):
                offset = pl.multiple_of(flags[1 + a] * span, span)
                scratch[pl.ds(offset, span), :] = refs[a][u * H + h]
            out_ref[h, u * rows : (u + 1) * rows, :] = scratch[...].T


def turn(flags, pieces, parts, group):
    span, rows = pieces[0].shape[1:]

    def body(flags_ref, *refs):
        turn_kernel(flags_ref, *refs, parts=parts, group=group)

    return pl.pallas_call(
        body,
        grid_spec=pltpu.PrefetchScalarGridSpec(
            num_scalar_prefetch=1,
            grid=(1,),
            in_specs=[pl.BlockSpec(p.shape, lambda i, f: (0, 0, 0)) for p in pieces],
            out_specs=pl.BlockSpec((H, parts * rows, group * span), lambda i, f: (0, 0, 0)),
            scratch_shapes=[pltpu.VMEM((group * span, rows), F32)],
        ),
        out_shape=jax.ShapeDtypeStruct((H, parts * rows, group * span), F32),
        name="turn",
    )(flags, *pieces)


def prepare_kernel(w_ref, wqgv_ref, wk_ref):
    inner = H * HD
    for place, part in enumerate((0, 3, 2)):
        block = w_ref[:, part * inner : (part + 1) * inner]
        wqgv_ref[place * inner : (place + 1) * inner, :] = block.astype(F32).T.astype(BF16)
    wk_ref[...] = w_ref[:, inner : 2 * inner]


def prepare(w_proj):
    channels = w_proj.shape[0]
    inner = H * HD
    return pl.pallas_call(
        prepare_kernel,
        out_shape=[
            jax.ShapeDtypeStruct((3 * inner, channels), BF16),
            jax.ShapeDtypeStruct((channels, inner), BF16),
        ],
        name="prepare",
    )(w_proj)


def attend_kernel(flags, x_ref, wqgv_ref, wk_ref, wout_ref, gb_ref, ob_ref, *rest, parts, aliased):
    n_refs = rest[:parts]
    bias_ref = rest[parts]
    rest = rest[parts + 1 + aliased :]
    out_ref, update_s, q_s, g_s, k_s, v_s, a_s, s_even, s_odd, p_even, p_odd = rest
    s_s = (s_even, s_odd)
    p_s = (p_even, p_odd)
    rows, cols, channels = x_ref.shape
    inner = H * HD
    keys = parts * rows
    wide = 2 * rows
    active = flags[0] > 0

    def project(t):
        own = n_refs[0][2 * t : 2 * t + 2].reshape(wide, channels)
        made = lax.dot_general(wqgv_ref[...], own, NT, preferred_element_type=F32)
        for e in range(2):
            lanes = slice(e * rows, (e + 1) * rows)
            q_s[2 * t + e] = (made[:inner, lanes] * HD ** (-0.5)).astype(BF16)
            g_s[2 * t + e] = jax.nn.sigmoid(made[inner : 2 * inner, lanes] + gb_ref[...])
            v_s[2 * t + e, :, 0:rows] = made[2 * inner :, lanes].astype(BF16)
        for u in range(1, parts):
            other = n_refs[u][2 * t : 2 * t + 2].reshape(wide, channels)
            made = lax.dot_general(wqgv_ref[2 * inner :], other, NT, preferred_element_type=F32)
            for e in range(2):
                v_s[2 * t + e, :, u * rows : (u + 1) * rows] = made[:, e * rows : (e + 1) * rows].astype(BF16)
        for u in range(parts):
            block = n_refs[u][2 * t : 2 * t + 2].reshape(wide, channels)
            made = jnp.dot(block, wk_ref[...], preferred_element_type=F32).astype(BF16)
            for e in range(2):
                k_s[2 * t + e, u * rows : (u + 1) * rows, :] = made[e * rows : (e + 1) * rows]

    def score(j, pair):
        q = q_s[j]
        columns = []
        for h in (2 * pair, 2 * pair + 1):
            blocks = [q[h * HD : (h + 1) * HD]]
            if h:
                blocks.insert(0, jnp.zeros((h * HD, rows), BF16))
            if h < H - 1:
                blocks.append(jnp.zeros(((H - 1 - h) * HD, rows), BF16))
            columns.append(jnp.concatenate(blocks, axis=0))
        both = jnp.concatenate(columns, axis=1)
        s_s[j % 2][:, pair * wide : (pair + 1) * wide] = jnp.dot(k_s[j], both, preferred_element_type=F32)

    def soften(j, h):
        scores = s_s[j % 2][:, h * rows : (h + 1) * rows] + bias_ref[h]
        top = jnp.max(scores, axis=0, keepdims=True)
        p_s[j % 2][:, h * rows : (h + 1) * rows] = jnp.exp(scores - top).astype(BF16)

    def mix(j, pair):
        lifted = jnp.concatenate([v_s[j, wide_head(pair)], jnp.ones((16, keys), BF16)], axis=0)
        mixed = jnp.dot(lifted, p_s[j % 2][:, pair * wide : (pair + 1) * wide], preferred_element_type=F32)
        for e in range(2):
            h = 2 * pair + e
            lanes = slice(e * rows, (e + 1) * rows)
            part = mixed[e * HD : (e + 1) * HD, lanes] / mixed[2 * HD : 2 * HD + 1, lanes]
            a_s[j, h * HD : (h + 1) * HD] = part.astype(BF16)

    def wide_head(pair):
        return slice(2 * pair * HD, (2 * pair + 2) * HD)

    def close(j):
        gated = (g_s[j] * a_s[j].astype(F32)).astype(BF16)
        update = lax.dot_general(gated, wout_ref[...], TN, preferred_element_type=F32) + ob_ref[...]
        update_s[pl.ds(j, rows, stride=cols), :] = update

    @pl.when(active)
    def _():
        for t in range(cols // 2):
            project(t)
        for t in range(-1, cols + 2):
            for pair in range(H // 2):
                if 0 <= t + 1 < cols:
                    score(t + 1, pair)
                if 0 <= t < cols:
                    soften(t, 2 * pair)
                    soften(t, 2 * pair + 1)
                if 0 <= t - 1 < cols:
                    mix(t - 1, pair)
            if 0 <= t - 2 < cols:
                close(t - 2)
        step = 16

        def finish(index, carried):
            start = index * step
            update = update_s[pl.ds(start * cols, step * cols), :].reshape(step, cols, channels)
            out_ref[pl.ds(start, step)] = (x_ref[pl.ds(start, step)].astype(F32) + update).astype(BF16)
            return carried

        lax.fori_loop(0, rows // step, finish, 0, unroll=2)

    @pl.when(jnp.logical_not(active))
    def _():
        out_ref[...] = x_ref[...]


def attend_chunk(flags, x, weights, norms, bias, out_in, first, cols):
    rows, cols_dev, channels = x.shape
    inner = H * HD
    parts = len(norms)
    keys = parts * rows
    steps = cols // SUB
    base = first // SUB
    whole = lambda a: pl.BlockSpec(a.shape, lambda i, f, nd=a.ndim: (0,) * nd)
    in_specs = [pl.BlockSpec((rows, SUB, channels), lambda i, f: (0, base + i, 0))]
    in_specs += [whole(a) for a in weights]
    in_specs += [pl.BlockSpec((SUB, rows, channels), lambda i, f: (i, 0, 0)) for _ in norms]
    in_specs.append(whole(bias))
    operands = [flags, x, *weights, *norms, bias]
    aliases = {}
    if out_in is not None:
        in_specs.append(pl.BlockSpec(memory_space=ANY))
        aliases = {len(operands): 0}
        operands.append(out_in)
    aliased = len(aliases)

    def body(flags_ref, *refs):
        attend_kernel(flags_ref, *refs, parts=parts, aliased=aliased)

    return pl.pallas_call(
        body,
        grid_spec=pltpu.PrefetchScalarGridSpec(
            num_scalar_prefetch=1,
            grid=(steps,),
            in_specs=in_specs,
            out_specs=pl.BlockSpec((rows, SUB, channels), lambda i, f: (0, base + i, 0)),
            scratch_shapes=[
                pltpu.VMEM((rows * SUB, channels), F32),
                pltpu.VMEM((SUB, inner, rows), BF16),
                pltpu.VMEM((SUB, inner, rows), F32),
                pltpu.VMEM((SUB, keys, inner), BF16),
                pltpu.VMEM((SUB, inner, keys), BF16),
                pltpu.VMEM((SUB, inner, rows), BF16),
                pltpu.VMEM((keys, H * rows), F32),
                pltpu.VMEM((keys, H * rows), F32),
                pltpu.VMEM((keys, H * rows), BF16),
                pltpu.VMEM((keys, H * rows), BF16),
            ],
        ),
        out_shape=jax.ShapeDtypeStruct((rows, cols_dev, channels), BF16),
        input_output_aliases=aliases,
        cost_estimate=pl.CostEstimate(
            flops=16 * cols * H * rows * keys * 128,
            bytes_accessed=2 * cols * channels * (2 * rows + keys),
            transcendentals=cols * H * rows * keys,
        ),
    )(*operands)


def run_pattern(valid, row_count, col_count, args):
    pair_rep, ln_gain, ln_shift, w_proj, gate_bias, w_bias, w_out, out_bias = args
    rows_dev, cols_dev, channels = pair_rep.shape
    inner = H * HD
    group = rows_dev // cols_dev
    nv = len(valid)
    row_id = lax.axis_index("row")
    col_id = lax.axis_index("col")
    block_id = col_id // group
    inner_id = col_id % group
    axes = ("row", "col")

    def at(row, block, a):
        return row * col_count + block * group + a

    def move(x, pairs, blocks=valid):
        full = [(at(s, b, i), at(d, b, i)) for (s, d) in pairs for b in blocks for i in range(group)]
        return lax.ppermute(x, axes, full)

    row_ok = jnp.zeros((), jnp.bool_)
    col_ok = jnp.zeros((), jnp.bool_)
    row_place = jnp.zeros((), jnp.int32)
    block_place = jnp.zeros((), jnp.int32)
    for p, b in enumerate(valid):
        row_ok = row_ok | (row_id == b)
        col_ok = col_ok | (block_id == b)
        row_place = jnp.where(row_id == b, p, row_place)
        block_place = jnp.where(block_id == b, p, block_place)
    active = (row_ok & col_ok).astype(jnp.int32)
    flags = jnp.stack([active] + [((inner_id - a) % group).astype(jnp.int32) for a in range(group)])

    gain = ln_gain.reshape(1, channels)
    shift = ln_shift.reshape(1, channels)
    wb = w_bias.T
    wqgv, wk = prepare(w_proj)
    weights = (wqgv, wk, w_out, gate_bias.reshape(inner, 1), out_bias.reshape(1, channels))

    chunks = chunk_list(cols_dev, EIGHTHS.get(nv, (4, 4)))
    norms = []
    bias = None
    for first, cols in chunks:
        n_c, bias = norm_chunk(pair_rep, gain, shift, wb, bias, first, cols)
        norms.append(n_c)

    held = [bias]
    for t in range(1, nv):
        pairs = []
        for p in range(nv):
            for r in valid:
                for i in range(group):
                    pairs.append((at(r, valid[p], i), at(r, valid[(p + t) % nv], i)))
        held.append(lax.ppermute(bias, axes, pairs))

    held[0], flags = lax.optimization_barrier((held[0], flags))

    def pick(place):
        back = (block_place - place) % nv
        chosen = held[0]
        for t in range(1, nv):
            chosen = jnp.where(back == t, held[t], chosen)
        return chosen

    picked = [pick((row_place + u) % nv) for u in range(nv)]
    pieces = [picked[0]]
    for u in range(1, nv):
        pairs = [(valid[p], valid[(p + u) % nv]) for p in range(nv)]
        pieces.append(move(picked[u], pairs))
    stacked = jnp.concatenate(pieces, axis=0)
    gathered = [stacked]
    for a in range(1, group):
        pairs = [(at(r, b, i), at(r, b, (i + a) % group)) for r in valid for b in valid for i in range(group)]
        gathered.append(lax.ppermute(stacked, axes, pairs))
    bias_t = turn(flags, gathered, nv, group)

    square = row_count == 4
    ring = [[(valid[p], valid[(p + u) % nv]) for p in range(nv)] for u in range(nv)]
    parts = [[n_c] for n_c in norms]
    for index in range(len(chunks)):
        early = picked if nv == 2 else pieces
        source = after(norms[index], *early[1:]) if index else norms[index]
        for u in range(1, nv):
            late = [(s, d) for s, d in ring[u] if square and (s ^ d) == 3 and (s ^ 1) in valid]
            if late:
                there = [(s, s ^ 2) if (s, d) in late else (s, d) for s, d in ring[u]]
                got = move(source, there)
            else:
                got = move(source, ring[u])
            if late:
                back = [(s ^ 2, d) if (s, d) in late else (d, d) for s, d in ring[u]]
                gate = (bias_t,) if index else tuple(pieces[1:])
                got = move(after(got, *gate), back)
            parts[index].append(got)

    out = None
    for index, (first, cols) in enumerate(chunks):
        out = attend_chunk(flags, pair_rep, weights, parts[index], bias_t, out, first, cols)
    return out


def chunk_list(cols_dev, eighths):
    lengths = [cols_dev * part // 8 for part in eighths]
    if any(length % SUB for length in lengths):
        lengths = [16] * (cols_dev // 16)
    return [(sum(lengths[:i]), length) for i, length in enumerate(lengths)]


def after(value, *others):
    return lax.optimization_barrier((value, *others))[0] if others else value


def patterns(blocks):
    fixed = {0, blocks // 2}
    free = [b for b in range(blocks) if b not in fixed]
    found = []
    for bits in itertools.product((0, 1), repeat=len(free)):
        if sum(bits) < len(free):
            found.append((bits, tuple(sorted(fixed | {b for b, on in zip(free, bits) if on}))))
    return free, found


def shards(pair_rep, ln_gain, ln_shift, w_proj, gate_bias, w_bias, w_out, out_bias, block_valid):
    row_count = lax.axis_size("row")
    col_count = lax.axis_size("col")
    args = (pair_rep, ln_gain, ln_shift, w_proj, gate_bias, w_bias, w_out, out_bias)
    free, found = patterns(block_valid.shape[0])
    index = jnp.zeros((), jnp.int32)
    for place, (bits, _) in enumerate(found):
        same = jnp.ones((), jnp.bool_)
        for b, on in zip(free, bits):
            same = same & ((block_valid[b] > 0) == bool(on))
        index = jnp.where(same, place, index)

    def branch(valid):
        def run(operands):
            return run_pattern(valid, row_count, col_count, operands)

        return run

    branches = [branch(valid) for _, valid in found]
    return lax.switch(index, branches, args)


def layer_norm(values, ln_gain, ln_shift):
    widened = values.astype(jnp.float32)
    average = jnp.mean(widened, axis=-1, keepdims=True)
    spread = jnp.mean((widened - average) ** 2, axis=-1, keepdims=True)
    return ((widened - average) * lax.rsqrt(spread + 1e-05) * ln_gain + ln_shift).astype(
        jnp.bfloat16
    )


def residue_valid(block_valid, residues):
    blocks = block_valid.shape[0]
    block_width = residues // blocks
    owner = jnp.arange(residues, dtype=jnp.int32) // block_width
    matches = (owner[:, None] == jnp.arange(blocks, dtype=jnp.int32)[None, :]).astype(jnp.float32)
    return jnp.sum(matches * block_valid.astype(jnp.float32)[None, :], axis=1)


def start_state(width_j, query_count):
    running_max = jnp.full((H, width_j, query_count), -1e30, jnp.float32)
    denominator = jnp.zeros((H, width_j, query_count), jnp.float32)
    weighted = jnp.zeros((query_count, width_j, H, HD), jnp.float32)
    return (running_max, denominator, weighted)


def finish(carried):
    _, denominator, weighted = carried
    mixed = weighted / jnp.transpose(denominator, (2, 1, 0))[..., None]
    return mixed.reshape(mixed.shape[0], mixed.shape[1], H * HD).astype(jnp.bfloat16)


def fold_keys(carried, queries, key_rows, values, bias_part, validity):
    query_count, width_j, _ = queries.shape
    key_count = key_rows.shape[0]
    key_step = math.gcd(key_count, BLK)
    steps = key_count // key_step
    query_heads = queries.reshape(query_count, width_j, H, HD)
    key_blocks = key_rows.reshape(steps, key_step, width_j, H, HD)
    value_blocks = values.reshape(steps, key_step, width_j, H, HD)
    bias_blocks = jnp.transpose(bias_part.reshape(H, query_count, steps, key_step), (2, 0, 1, 3))
    mask_blocks = validity.reshape(steps, key_step)

    def update(carried_in, operands):
        key_part, value_part, bias_block, mask_part = operands
        running_max, denominator, weighted = carried_in
        scores = jnp.einsum(
            "ijhd,kjhd->hjik", query_heads, key_part, preferred_element_type=jnp.float32
        )
        scores = scores + bias_block[:, None, :, :]
        scores = jnp.where(mask_part[None, None, None, :] > 0, scores, jnp.float32(-1e30))
        renewed = jnp.maximum(running_max, jnp.max(scores, axis=-1))
        weights = jnp.exp(scores - renewed[..., None]) * mask_part[None, None, None, :]
        shrink = jnp.exp(running_max - renewed)
        denominator = denominator * shrink + jnp.sum(weights, axis=-1)
        product = jnp.einsum(
            "hjik,kjhd->ijhd",
            weights.astype(jnp.bfloat16),
            value_part,
            preferred_element_type=jnp.float32,
        )
        weighted = weighted * jnp.transpose(shrink, (2, 1, 0))[..., None] + product
        return (renewed, denominator, weighted)

    def scan_step(carried_in, operands):
        renewed = lax.cond(
            jnp.max(operands[3]) > 0, update, lambda kept, ignored: kept, carried_in, operands
        )
        return (renewed, None)

    result, _ = lax.scan(scan_step, carried, (key_blocks, value_blocks, bias_blocks, mask_blocks))
    return result


def general_shards(pair_rep, ln_gain, ln_shift, w_proj, gate_bias, w_bias, w_out, out_bias, block_valid):
    rows_dev, cols_dev, channels = pair_rep.shape
    row_count = lax.axis_size("row")
    row_id = lax.axis_index("row")
    col_id = lax.axis_index("col")
    residues = rows_dev * row_count
    inner = H * HD
    query_scale = HD ** (-0.5)
    validity = residue_valid(block_valid, residues)
    normed = layer_norm(pair_rep, ln_gain, ln_shift)
    flat_rows = normed.reshape(rows_dev * cols_dev, channels)
    bias_local = jnp.dot(flat_rows, w_bias, preferred_element_type=jnp.float32)
    bias_local = jnp.transpose(bias_local.reshape(rows_dev, cols_dev, H), (2, 1, 0))
    bias_cols = lax.all_gather(bias_local, "row", axis=2, tiled=True)
    regrouped = lax.all_to_all(normed, "row", split_axis=1, concat_axis=0, tiled=True)
    width_j = regrouped.shape[1]
    projected = jnp.dot(
        regrouped.reshape(residues * width_j, channels),
        w_proj[:, : 3 * inner],
        preferred_element_type=jnp.float32,
    )
    projected = projected.reshape(residues, width_j, 3 * inner)
    queries = (projected[..., :inner] * query_scale).astype(jnp.bfloat16)
    key_rows = projected[..., inner : 2 * inner].astype(jnp.bfloat16)
    values = projected[..., 2 * inner :].astype(jnp.bfloat16)
    bias_piece = lax.all_gather(bias_cols, "col", axis=1, tiled=True)
    span_rows = bias_piece.shape[1]
    query_block = math.gcd(span_rows, cols_dev)
    block_count = span_rows // query_block
    query_rows = queries
    query_rows = query_rows.reshape(block_count, query_block, width_j, inner)
    bias_blocks = jnp.transpose(
        bias_piece.reshape(H, block_count, query_block, residues), (1, 0, 2, 3)
    )

    def one_block(operands):
        query_part, bias_part = operands
        carried = fold_keys(
            start_state(width_j, query_block), query_part, key_rows, values, bias_part, validity
        )
        return finish(carried)

    results = lax.map(one_block, (query_rows, bias_blocks))
    gathered = results.reshape(span_rows, width_j, inner)
    attended = lax.all_to_all(gathered, "row", split_axis=0, concat_axis=1, tiled=True)
    gate_pre = jnp.dot(flat_rows, w_proj[:, 3 * inner :], preferred_element_type=jnp.float32)
    gate_pre = gate_pre.reshape(rows_dev, cols_dev, inner)
    gate_act = jax.nn.sigmoid(gate_pre + gate_bias)
    gated_rows = (gate_act * attended.astype(jnp.float32)).astype(jnp.bfloat16)
    update = jnp.dot(
        gated_rows.reshape(rows_dev * cols_dev, inner), w_out, preferred_element_type=jnp.float32
    )
    update = update.reshape(rows_dev, cols_dev, channels) + out_bias
    row_valid = lax.dynamic_slice_in_dim(validity, row_id * rows_dev, rows_dev, 0)
    col_valid = lax.dynamic_slice_in_dim(validity, col_id * cols_dev, cols_dev, 0)
    pair_mask = row_valid[:, None] * col_valid[None, :]
    return (pair_rep.astype(jnp.float32) + update * pair_mask[..., None]).astype(jnp.bfloat16)


def solution(mesh):
    def body(*args):
        pair_rep, block_valid = args[0], args[-1]
        blocks = block_valid.shape[0]
        rows_dev, cols_dev, _ = pair_rep.shape
        aligned = blocks == lax.axis_size("row") and rows_dev % cols_dev == 0 and cols_dev % 16 == 0
        if aligned and len(patterns(blocks)[1]) <= 4:
            return shards(*args)
        return general_shards(*args)

    return jax.shard_map(
        body,
        mesh=mesh,
        in_specs=(P("row", "col", None), P(), P(), P(), P(), P(), P(), P(), P()),
        out_specs=P("row", "col", None),
        check_vma=False,
    )
```

```python
import itertools
import math

import jax
import jax.numpy as jnp
from jax import lax
from jax.experimental import pallas as pl
from jax.experimental.pallas import tpu as pltpu
from jax.sharding import PartitionSpec as P


H = 4
HD = 32
BLK = 128


ANY = pl.ANY
NT = (((1,), (1,)), ((), ()))
TN = (((0,), (0,)), ((), ()))
F32 = jnp.float32
BF16 = jnp.bfloat16
SUB = 8
EIGHTHS = {2: (3, 3, 2), 3: (5, 3)}


def norm_kernel(x_ref, gain_ref, shift_ref, wb_ref, *rest):
    n_ref, bias_ref, scratch = rest[-3:]
    rows, cols, channels = x_ref.shape
    step = 8
    count = rows // step
    centred = {}
    spread = {}
    for t in range(count + 2):
        if t < count:
            widened = x_ref[t * step : (t + 1) * step].reshape(step * cols, channels).astype(F32)
            centred[t] = widened - jnp.mean(widened, axis=-1, keepdims=True)
        if 0 <= t - 1 < count:
            spread[t - 1] = jnp.mean(centred[t - 1] * centred[t - 1], axis=-1, keepdims=True)
        if 0 <= t - 2 < count:
            scaled = centred.pop(t - 2) * lax.rsqrt(spread.pop(t - 2) + 1e-05)
            scratch[(t - 2) * step * cols : (t - 1) * step * cols, :] = scaled * gain_ref[...] + shift_ref[...]
    for j in range(cols):
        column = scratch[pl.ds(j, rows, stride=cols), :].astype(BF16)
        n_ref[j] = column
        part = lax.dot_general(wb_ref[...], column, NT, preferred_element_type=F32)
        for h in range(H):
            bias_ref[h, j : j + 1, :] = part[h : h + 1, :]


def norm_chunk(x, gain, shift, wb, bias_in, first, cols):
    rows, cols_dev, channels = x.shape
    sub = 16 if cols % 16 == 0 and first % 16 == 0 else SUB
    steps = cols // sub
    base = first // sub
    in_specs = [
        pl.BlockSpec((rows, sub, channels), lambda i: (0, base + i, 0)),
        pl.BlockSpec((1, channels), lambda i: (0, 0)),
        pl.BlockSpec((1, channels), lambda i: (0, 0)),
        pl.BlockSpec(wb.shape, lambda i: (0, 0)),
    ]
    operands = [x, gain, shift, wb]
    aliases = {}
    if bias_in is not None:
        in_specs.append(pl.BlockSpec(memory_space=ANY))
        operands.append(bias_in)
        aliases = {4: 1}
    return pl.pallas_call(
        norm_kernel,
        grid=(steps,),
        in_specs=in_specs,
        out_specs=[
            pl.BlockSpec((sub, rows, channels), lambda i: (i, 0, 0)),
            pl.BlockSpec((H, sub, rows), lambda i: (0, base + i, 0)),
        ],
        out_shape=[
            jax.ShapeDtypeStruct((cols, rows, channels), BF16),
            jax.ShapeDtypeStruct((H, cols_dev, rows), F32),
        ],
        scratch_shapes=[pltpu.VMEM((rows * sub, channels), F32)],
        input_output_aliases=aliases,
        cost_estimate=pl.CostEstimate(
            flops=200 * rows * cols * channels, bytes_accessed=4 * rows * cols * channels, transcendentals=0
        ),
    )(*operands)


def turn_kernel(flags, *refs, parts, group):
    out_ref, scratch = refs[-2:]
    span, rows = refs[0].shape[1:]
    for u in range(parts):
        for h in range(H):
            for a in range(group):
                offset = pl.multiple_of(flags[1 + a] * span, span)
                scratch[pl.ds(offset, span), :] = refs[a][u * H + h]
            out_ref[h, u * rows : (u + 1) * rows, :] = scratch[...].T


def turn(flags, pieces, parts, group):
    span, rows = pieces[0].shape[1:]

    def body(flags_ref, *refs):
        turn_kernel(flags_ref, *refs, parts=parts, group=group)

    return pl.pallas_call(
        body,
        grid_spec=pltpu.PrefetchScalarGridSpec(
            num_scalar_prefetch=1,
            grid=(1,),
            in_specs=[pl.BlockSpec(p.shape, lambda i, f: (0, 0, 0)) for p in pieces],
            out_specs=pl.BlockSpec((H, parts * rows, group * span), lambda i, f: (0, 0, 0)),
            scratch_shapes=[pltpu.VMEM((group * span, rows), F32)],
        ),
        out_shape=jax.ShapeDtypeStruct((H, parts * rows, group * span), F32),
        name="turn",
    )(flags, *pieces)


def prepare_kernel(w_ref, wqgv_ref, wk_ref):
    inner = H * HD
    for place, part in enumerate((0, 3, 2)):
        block = w_ref[:, part * inner : (part + 1) * inner]
        wqgv_ref[place * inner : (place + 1) * inner, :] = block.astype(F32).T.astype(BF16)
    wk_ref[...] = w_ref[:, inner : 2 * inner]


def prepare(w_proj):
    channels = w_proj.shape[0]
    inner = H * HD
    return pl.pallas_call(
        prepare_kernel,
        out_shape=[
            jax.ShapeDtypeStruct((3 * inner, channels), BF16),
            jax.ShapeDtypeStruct((channels, inner), BF16),
        ],
        name="prepare",
    )(w_proj)


def attend_kernel(flags, x_ref, wqgv_ref, wk_ref, wout_ref, gb_ref, ob_ref, *rest, parts, aliased, late, late_flag):
    n_refs = rest[:parts]
    late_refs = rest[parts : parts + len(late)]
    rest = rest[parts + len(late) :]
    bias_ref = rest[0]
    rest = rest[1 + aliased :]
    out_ref, update_s, q_s, g_s, k_s, v_s, a_s, s_even, s_odd, p_even, p_odd = rest
    s_s = (s_even, s_odd)
    p_s = (p_even, p_odd)
    rows, cols, channels = x_ref.shape
    inner = H * HD
    keys = parts * rows
    wide = 2 * rows
    active = flags[0] > 0

    def project(t):
        blocks = [n_ref[2 * t : 2 * t + 2].reshape(wide, channels) for n_ref in n_refs]
        for u, late_ref in zip(late, late_refs):
            other = late_ref[2 * t : 2 * t + 2].reshape(wide, channels)
            blocks[u] = jnp.where(flags[late_flag] > 0, other, blocks[u])
        made = lax.dot_general(wqgv_ref[...], blocks[0], NT, preferred_element_type=F32)
        for e in range(2):
            lanes = slice(e * rows, (e + 1) * rows)
            q_s[2 * t + e] = (made[:inner, lanes] * HD ** (-0.5)).astype(BF16)
            g_s[2 * t + e] = jax.nn.sigmoid(made[inner : 2 * inner, lanes] + gb_ref[...])
            v_s[2 * t + e, :, 0:rows] = made[2 * inner :, lanes].astype(BF16)
        for u in range(1, parts):
            made = lax.dot_general(wqgv_ref[2 * inner :], blocks[u], NT, preferred_element_type=F32)
            for e in range(2):
                v_s[2 * t + e, :, u * rows : (u + 1) * rows] = made[:, e * rows : (e + 1) * rows].astype(BF16)
        for u in range(parts):
            made = jnp.dot(blocks[u], wk_ref[...], preferred_element_type=F32).astype(BF16)
            for e in range(2):
                k_s[2 * t + e, u * rows : (u + 1) * rows, :] = made[e * rows : (e + 1) * rows]

    def score(j, pair):
        q = q_s[j]
        columns = []
        for h in (2 * pair, 2 * pair + 1):
            blocks = [q[h * HD : (h + 1) * HD]]
            if h:
                blocks.insert(0, jnp.zeros((h * HD, rows), BF16))
            if h < H - 1:
                blocks.append(jnp.zeros(((H - 1 - h) * HD, rows), BF16))
            columns.append(jnp.concatenate(blocks, axis=0))
        both = jnp.concatenate(columns, axis=1)
        s_s[j % 2][:, pair * wide : (pair + 1) * wide] = jnp.dot(k_s[j], both, preferred_element_type=F32)

    def soften(j, h):
        scores = s_s[j % 2][:, h * rows : (h + 1) * rows] + bias_ref[h]
        top = jnp.max(scores, axis=0, keepdims=True)
        p_s[j % 2][:, h * rows : (h + 1) * rows] = jnp.exp(scores - top).astype(BF16)

    def mix(j, pair):
        lifted = jnp.concatenate([v_s[j, wide_head(pair)], jnp.ones((16, keys), BF16)], axis=0)
        mixed = jnp.dot(lifted, p_s[j % 2][:, pair * wide : (pair + 1) * wide], preferred_element_type=F32)
        for e in range(2):
            h = 2 * pair + e
            lanes = slice(e * rows, (e + 1) * rows)
            part = mixed[e * HD : (e + 1) * HD, lanes] / mixed[2 * HD : 2 * HD + 1, lanes]
            a_s[j, h * HD : (h + 1) * HD] = part.astype(BF16)

    def wide_head(pair):
        return slice(2 * pair * HD, (2 * pair + 2) * HD)

    def close(j):
        gated = (g_s[j] * a_s[j].astype(F32)).astype(BF16)
        update = lax.dot_general(gated, wout_ref[...], TN, preferred_element_type=F32) + ob_ref[...]
        update_s[pl.ds(j, rows, stride=cols), :] = update

    @pl.when(active)
    def _():
        for t in range(cols // 2):
            project(t)
        for t in range(-1, cols + 2):
            for pair in range(H // 2):
                if 0 <= t + 1 < cols:
                    score(t + 1, pair)
                if 0 <= t < cols:
                    soften(t, 2 * pair)
                    soften(t, 2 * pair + 1)
                if 0 <= t - 1 < cols:
                    mix(t - 1, pair)
            if 0 <= t - 2 < cols:
                close(t - 2)
        step = 16

        def finish(index, carried):
            start = index * step
            update = update_s[pl.ds(start * cols, step * cols), :].reshape(step, cols, channels)
            out_ref[pl.ds(start, step)] = (x_ref[pl.ds(start, step)].astype(F32) + update).astype(BF16)
            return carried

        lax.fori_loop(0, rows // step, finish, 0, unroll=2)

    @pl.when(jnp.logical_not(active))
    def _():
        out_ref[...] = x_ref[...]


def attend_chunk(flags, x, weights, norms, relayed, late_flag, bias, out_in, first, cols):
    rows, cols_dev, channels = x.shape
    inner = H * HD
    parts = len(norms)
    keys = parts * rows
    steps = cols // SUB
    base = first // SUB
    whole = lambda a: pl.BlockSpec(a.shape, lambda i, f, nd=a.ndim: (0,) * nd)
    in_specs = [pl.BlockSpec((rows, SUB, channels), lambda i, f: (0, base + i, 0))]
    in_specs += [whole(a) for a in weights]
    late = tuple(relayed)
    blocks = [*norms, *relayed.values()]
    in_specs += [pl.BlockSpec((SUB, rows, channels), lambda i, f: (i, 0, 0)) for _ in blocks]
    in_specs.append(whole(bias))
    operands = [flags, x, *weights, *blocks, bias]
    aliases = {}
    if out_in is not None:
        in_specs.append(pl.BlockSpec(memory_space=ANY))
        aliases = {len(operands): 0}
        operands.append(out_in)
    aliased = len(aliases)

    def body(flags_ref, *refs):
        attend_kernel(
            flags_ref, *refs, parts=parts, aliased=aliased, late=late, late_flag=late_flag
        )

    return pl.pallas_call(
        body,
        grid_spec=pltpu.PrefetchScalarGridSpec(
            num_scalar_prefetch=1,
            grid=(steps,),
            in_specs=in_specs,
            out_specs=pl.BlockSpec((rows, SUB, channels), lambda i, f: (0, base + i, 0)),
            scratch_shapes=[
                pltpu.VMEM((rows * SUB, channels), F32),
                pltpu.VMEM((SUB, inner, rows), BF16),
                pltpu.VMEM((SUB, inner, rows), F32),
                pltpu.VMEM((SUB, keys, inner), BF16),
                pltpu.VMEM((SUB, inner, keys), BF16),
                pltpu.VMEM((SUB, inner, rows), BF16),
                pltpu.VMEM((keys, H * rows), F32),
                pltpu.VMEM((keys, H * rows), F32),
                pltpu.VMEM((keys, H * rows), BF16),
                pltpu.VMEM((keys, H * rows), BF16),
            ],
        ),
        out_shape=jax.ShapeDtypeStruct((rows, cols_dev, channels), BF16),
        input_output_aliases=aliases,
        cost_estimate=pl.CostEstimate(
            flops=16 * cols * H * rows * keys * 128,
            bytes_accessed=2 * cols * channels * (2 * rows + keys),
            transcendentals=cols * H * rows * keys,
        ),
    )(*operands)


def run_pattern(valid, row_count, col_count, args):
    pair_rep, ln_gain, ln_shift, w_proj, gate_bias, w_bias, w_out, out_bias = args
    rows_dev, cols_dev, channels = pair_rep.shape
    inner = H * HD
    group = rows_dev // cols_dev
    nv = len(valid)
    row_id = lax.axis_index("row")
    col_id = lax.axis_index("col")
    block_id = col_id // group
    inner_id = col_id % group
    axes = ("row", "col")

    def at(row, block, a):
        return row * col_count + block * group + a

    def move(x, pairs, blocks=valid):
        full = [(at(s, b, i), at(d, b, i)) for (s, d) in pairs for b in blocks for i in range(group)]
        return lax.ppermute(x, axes, full)

    row_ok = jnp.zeros((), jnp.bool_)
    col_ok = jnp.zeros((), jnp.bool_)
    row_place = jnp.zeros((), jnp.int32)
    block_place = jnp.zeros((), jnp.int32)
    for p, b in enumerate(valid):
        row_ok = row_ok | (row_id == b)
        col_ok = col_ok | (block_id == b)
        row_place = jnp.where(row_id == b, p, row_place)
        block_place = jnp.where(block_id == b, p, block_place)
    active = (row_ok & col_ok).astype(jnp.int32)
    square = row_count == 4
    ring = [[(valid[p], valid[(p + u) % nv]) for p in range(nv)] for u in range(nv)]
    late_moves = [
        [(s, d) for s, d in ring[u] if u and square and (s ^ d) == 3 and (s ^ 1) in valid] for u in range(nv)
    ]
    relayed_row = jnp.zeros((), jnp.bool_)
    for moves in late_moves:
        for _, d in moves:
            relayed_row = relayed_row | (row_id == d)
    flags = [active] + [((inner_id - a) % group).astype(jnp.int32) for a in range(group)]
    flags = jnp.stack(flags + [relayed_row.astype(jnp.int32)])

    gain = ln_gain.reshape(1, channels)
    shift = ln_shift.reshape(1, channels)
    wb = w_bias.T
    wqgv, wk = prepare(w_proj)
    weights = (wqgv, wk, w_out, gate_bias.reshape(inner, 1), out_bias.reshape(1, channels))

    chunks = chunk_list(cols_dev, EIGHTHS.get(nv, (4, 4)))
    norms = []
    bias = None
    for first, cols in chunks:
        n_c, bias = norm_chunk(pair_rep, gain, shift, wb, bias, first, cols)
        norms.append(n_c)

    held = [bias]
    for t in range(1, nv):
        pairs = []
        for p in range(nv):
            for r in valid:
                for i in range(group):
                    pairs.append((at(r, valid[p], i), at(r, valid[(p + t) % nv], i)))
        held.append(lax.ppermute(bias, axes, pairs))

    held[0], flags, gate_column = lax.optimization_barrier((held[0], flags, weights[3]))
    weights = (*weights[:3], gate_column, weights[4])

    def pick(place):
        back = (block_place - place) % nv
        chosen = held[0]
        for t in range(1, nv):
            chosen = jnp.where(back == t, held[t], chosen)
        return chosen

    picked = [pick((row_place + u) % nv) for u in range(nv)]
    pieces = [picked[0]]
    for u in range(1, nv):
        pairs = [(valid[p], valid[(p + u) % nv]) for p in range(nv)]
        pieces.append(move(picked[u], pairs))
    stacked = jnp.concatenate(pieces, axis=0)
    gathered = [stacked]
    for a in range(1, group):
        pairs = [(at(r, b, i), at(r, b, (i + a) % group)) for r in valid for b in valid for i in range(group)]
        gathered.append(lax.ppermute(stacked, axes, pairs))
    bias_t = turn(flags, gathered, nv, group)

    parts = [[n_c] for n_c in norms]
    relayed = [{} for _ in chunks]
    for index in range(len(chunks)):
        early = picked if nv == 2 else pieces
        source = after(norms[index], *early[1:]) if index else norms[index]
        for u in range(1, nv):
            late = late_moves[u]
            there = [(s, s ^ 2) if (s, d) in late else (s, d) for s, d in ring[u]]
            got = move(source, there)
            if late:
                gate = (bias_t,) if index else tuple(picked[1:])
                relayed[index][u] = move(after(got, *gate), [(s ^ 2, d) for s, d in late])
            parts[index].append(got)

    out = None
    for index, (first, cols) in enumerate(chunks):
        out = attend_chunk(flags, pair_rep, weights, parts[index], relayed[index], group + 1, bias_t, out, first, cols)
    return out


def chunk_list(cols_dev, eighths):
    lengths = [cols_dev * part // 8 for part in eighths]
    if any(length % SUB for length in lengths):
        lengths = [16] * (cols_dev // 16)
    return [(sum(lengths[:i]), length) for i, length in enumerate(lengths)]


def after(value, *others):
    return lax.optimization_barrier((value, *others))[0] if others else value


def patterns(blocks):
    fixed = {0, blocks // 2}
    free = [b for b in range(blocks) if b not in fixed]
    found = []
    for bits in itertools.product((0, 1), repeat=len(free)):
        if sum(bits) < len(free):
            found.append((bits, tuple(sorted(fixed | {b for b, on in zip(free, bits) if on}))))
    return free, found


def shards(pair_rep, ln_gain, ln_shift, w_proj, gate_bias, w_bias, w_out, out_bias, block_valid):
    row_count = lax.axis_size("row")
    col_count = lax.axis_size("col")
    args = (pair_rep, ln_gain, ln_shift, w_proj, gate_bias, w_bias, w_out, out_bias)
    free, found = patterns(block_valid.shape[0])
    index = jnp.zeros((), jnp.int32)
    for place, (bits, _) in enumerate(found):
        same = jnp.ones((), jnp.bool_)
        for b, on in zip(free, bits):
            same = same & ((block_valid[b] > 0) == bool(on))
        index = jnp.where(same, place, index)

    def branch(valid):
        def run(operands):
            return run_pattern(valid, row_count, col_count, operands)

        return run

    branches = [branch(valid) for _, valid in found]
    return lax.switch(index, branches, args)


def layer_norm(values, ln_gain, ln_shift):
    widened = values.astype(jnp.float32)
    average = jnp.mean(widened, axis=-1, keepdims=True)
    spread = jnp.mean((widened - average) ** 2, axis=-1, keepdims=True)
    return ((widened - average) * lax.rsqrt(spread + 1e-05) * ln_gain + ln_shift).astype(
        jnp.bfloat16
    )


def residue_valid(block_valid, residues):
    blocks = block_valid.shape[0]
    block_width = residues // blocks
    owner = jnp.arange(residues, dtype=jnp.int32) // block_width
    matches = (owner[:, None] == jnp.arange(blocks, dtype=jnp.int32)[None, :]).astype(jnp.float32)
    return jnp.sum(matches * block_valid.astype(jnp.float32)[None, :], axis=1)


def start_state(width_j, query_count):
    running_max = jnp.full((H, width_j, query_count), -1e30, jnp.float32)
    denominator = jnp.zeros((H, width_j, query_count), jnp.float32)
    weighted = jnp.zeros((query_count, width_j, H, HD), jnp.float32)
    return (running_max, denominator, weighted)


def finish(carried):
    _, denominator, weighted = carried
    mixed = weighted / jnp.transpose(denominator, (2, 1, 0))[..., None]
    return mixed.reshape(mixed.shape[0], mixed.shape[1], H * HD).astype(jnp.bfloat16)


def fold_keys(carried, queries, key_rows, values, bias_part, validity):
    query_count, width_j, _ = queries.shape
    key_count = key_rows.shape[0]
    key_step = math.gcd(key_count, BLK)
    steps = key_count // key_step
    query_heads = queries.reshape(query_count, width_j, H, HD)
    key_blocks = key_rows.reshape(steps, key_step, width_j, H, HD)
    value_blocks = values.reshape(steps, key_step, width_j, H, HD)
    bias_blocks = jnp.transpose(bias_part.reshape(H, query_count, steps, key_step), (2, 0, 1, 3))
    mask_blocks = validity.reshape(steps, key_step)

    def update(carried_in, operands):
        key_part, value_part, bias_block, mask_part = operands
        running_max, denominator, weighted = carried_in
        scores = jnp.einsum(
            "ijhd,kjhd->hjik", query_heads, key_part, preferred_element_type=jnp.float32
        )
        scores = scores + bias_block[:, None, :, :]
        scores = jnp.where(mask_part[None, None, None, :] > 0, scores, jnp.float32(-1e30))
        renewed = jnp.maximum(running_max, jnp.max(scores, axis=-1))
        weights = jnp.exp(scores - renewed[..., None]) * mask_part[None, None, None, :]
        shrink = jnp.exp(running_max - renewed)
        denominator = denominator * shrink + jnp.sum(weights, axis=-1)
        product = jnp.einsum(
            "hjik,kjhd->ijhd",
            weights.astype(jnp.bfloat16),
            value_part,
            preferred_element_type=jnp.float32,
        )
        weighted = weighted * jnp.transpose(shrink, (2, 1, 0))[..., None] + product
        return (renewed, denominator, weighted)

    def scan_step(carried_in, operands):
        renewed = lax.cond(
            jnp.max(operands[3]) > 0, update, lambda kept, ignored: kept, carried_in, operands
        )
        return (renewed, None)

    result, _ = lax.scan(
        scan_step, carried, (key_blocks, value_blocks, bias_blocks, mask_blocks)
    )
    return result


def general_shards(pair_rep, ln_gain, ln_shift, w_proj, gate_bias, w_bias, w_out, out_bias, block_valid):
    rows_dev, cols_dev, channels = pair_rep.shape
    row_count = lax.axis_size("row")
    row_id = lax.axis_index("row")
    col_id = lax.axis_index("col")
    residues = rows_dev * row_count
    inner = H * HD
    query_scale = HD ** (-0.5)
    validity = residue_valid(block_valid, residues)
    normed = layer_norm(pair_rep, ln_gain, ln_shift)
    flat_rows = normed.reshape(rows_dev * cols_dev, channels)
    bias_local = jnp.dot(flat_rows, w_bias, preferred_element_type=jnp.float32)
    bias_local = jnp.transpose(bias_local.reshape(rows_dev, cols_dev, H), (2, 1, 0))
    bias_cols = lax.all_gather(bias_local, "row", axis=2, tiled=True)
    regrouped = lax.all_to_all(normed, "row", split_axis=1, concat_axis=0, tiled=True)
    width_j = regrouped.shape[1]
    projected = jnp.dot(
        regrouped.reshape(residues * width_j, channels),
        w_proj[:, : 3 * inner],
        preferred_element_type=jnp.float32,
    )
    projected = projected.reshape(residues, width_j, 3 * inner)
    queries = (projected[..., :inner] * query_scale).astype(jnp.bfloat16)
    key_rows = projected[..., inner : 2 * inner].astype(jnp.bfloat16)
    values = projected[..., 2 * inner :].astype(jnp.bfloat16)
    bias_piece = lax.all_gather(bias_cols, "col", axis=1, tiled=True)
    span_rows = bias_piece.shape[1]
    query_block = math.gcd(span_rows, cols_dev)
    block_count = span_rows // query_block
    query_rows = queries
    query_rows = query_rows.reshape(block_count, query_block, width_j, inner)
    bias_blocks = jnp.transpose(
        bias_piece.reshape(H, block_count, query_block, residues), (1, 0, 2, 3)
    )

    def one_block(operands):
        query_part, bias_part = operands
        carried = fold_keys(
            start_state(width_j, query_block), query_part, key_rows, values, bias_part, validity
        )
        return finish(carried)

    results = lax.map(one_block, (query_rows, bias_blocks))
    gathered = results.reshape(span_rows, width_j, inner)
    attended = lax.all_to_all(gathered, "row", split_axis=0, concat_axis=1, tiled=True)
    gate_pre = jnp.dot(flat_rows, w_proj[:, 3 * inner :], preferred_element_type=jnp.float32)
    gate_pre = gate_pre.reshape(rows_dev, cols_dev, inner)
    gate_act = jax.nn.sigmoid(gate_pre + gate_bias)
    gated_rows = (gate_act * attended.astype(jnp.float32)).astype(jnp.bfloat16)
    update = jnp.dot(
        gated_rows.reshape(rows_dev * cols_dev, inner), w_out, preferred_element_type=jnp.float32
    )
    update = update.reshape(rows_dev, cols_dev, channels) + out_bias
    row_valid = lax.dynamic_slice_in_dim(validity, row_id * rows_dev, rows_dev, 0)
    col_valid = lax.dynamic_slice_in_dim(validity, col_id * cols_dev, cols_dev, 0)
    pair_mask = row_valid[:, None] * col_valid[None, :]
    return (pair_rep.astype(jnp.float32) + update * pair_mask[..., None]).astype(jnp.bfloat16)


def solution(mesh):
    def body(*args):
        pair_rep, block_valid = args[0], args[-1]
        blocks = block_valid.shape[0]
        rows_dev, cols_dev, _ = pair_rep.shape
        aligned = blocks == lax.axis_size("row") and rows_dev % cols_dev == 0 and cols_dev % 16 == 0
        if aligned and len(patterns(blocks)[1]) <= 4:
            return shards(*args)
        return general_shards(*args)

    return jax.shard_map(
        body,
        mesh=mesh,
        in_specs=(P("row", "col", None), P(), P(), P(), P(), P(), P(), P(), P()),
        out_specs=P("row", "col", None),
        check_vma=False,
    )
```
